512 devices in a mesh: tm: 128 (over z, y, core), space: 4 (over x).
Axes of the slice: x: 4, y: 8, z: 8, core: 2. Of those that a mesh axis runs over, the one named last changes fastest.
Arguments:
- right_side: float32 [512, 32, 256], P('tm', 'space'), may hold values from -24 to 24
- diffusion: float32 [32, 256], P('space'), may hold values from 0.5 to 4
- velocity: float32 [2, 32, 256], P(None, 'space'), may hold values from -0.5 to 0.5
Outputs:
- solution: float32 [512, 32, 256], P('tm', 'space')
- residual: float32 [512, 32, 256], P('tm', 'space')
The draws below stay inside these ranges and needn't reach their ends.
All inputs are finite; a program needn't handle non-finite values.
Results may differ from the reference program's by a relative error of at most 0.0003.
Values sent between devices are 32-bit elements; how exact they have to be, the bound alone decides.
A program may use at most 64 MiB of HBM per device.

```python
import math
import jax
import jax.numpy as jnp
from jax import lax

L = 512
NC = 256
KRYLOV = 3
SWEEPS = 3
NR = 32


def draw_right_side(key, part):
    base_key = jax.random.fold_in(key, 7)
    first = jax.random.fold_in(base_key, 0)
    noise = jax.random.normal(first, (L, NR, NC), jnp.float32)
    ramp = jnp.exp(jnp.arange(L, dtype=jnp.float32) * (math.log(3.0) / (L - 1)))[:, None, None]
    field = noise
    return jnp.clip(field * ramp, -24.0, 24.0)


def block_scale(key, dims, pieces, low, largest):
    loudness = 1.0
    for axis_at, shards_of in pieces:
        heights = jax.random.uniform(jax.random.fold_in(jax.random.fold_in(key, 6), axis_at), (shards_of,), jnp.float32, low / len(pieces), largest / len(pieces))
        loudness = loudness * jnp.repeat(jnp.exp(heights), dims[axis_at] // shards_of).reshape((-1,) + (1,) * (len(dims) - 1 - axis_at))
    return loudness


def setup_inputs(seed: int = 0) -> dict:
    splits = jax.random.split(jax.random.key(seed), 4)
    right_side = draw_right_side(jax.random.fold_in(splits[3], 71), 0)
    diffusion = jnp.clip(jnp.exp(math.log(4.0) - 2.0794415 * jax.random.uniform(splits[1], (NR, NC), jnp.float32) ** block_scale(splits[1], (NR, NC), ((0, 4),), -0.2, 0.2)), 0.5, 4.0)
    velocity = jnp.clip(jax.random.uniform(splits[2], (2, NR, NC), jnp.float32, -0.5, 0.5) * block_scale(splits[2], (2, NR, NC), ((1, 4),), -0.4, 0.0), -0.5, 0.5)
    return {"right_side": right_side, "diffusion": diffusion, "velocity": velocity}


alpha_corner = 0.05
damping = 0.8
epsilon = 1e-06

def stencil(field, padded, diffusion, velocity):
    north = padded[..., :-2, 1:-1]
    south = padded[..., 2:, 1:-1]
    west = padded[..., 1:-1, :-2]
    east = padded[..., 1:-1, 2:]
    return (1.0 + 4.0 * diffusion) * field - diffusion * (north + south + west + east) + velocity[0] * (east - west) + velocity[1] * (south - north)

def apply_step(field, diffusion, velocity):
    padded = jnp.pad(field, ((0, 0), (1, 1), (1, 1)))
    return stencil(field, padded, diffusion, velocity)

def system(field, diffusion, velocity):
    image = apply_step(field, diffusion, velocity)
    earlier = jnp.concatenate([jnp.zeros_like(field[:1]), field[:-1]], axis=0)
    return image - earlier

def divided(real_part, imag_part, diag_real, diag_imag, modulus):
    return (damping * (real_part * diag_real + imag_part * diag_imag) / modulus, damping * (imag_part * diag_real - real_part * diag_imag) / modulus)

def remainder(source_real, source_imag, image_real, image_imag, guess_real, guess_imag, shift_real, shift_imag):
    return (source_real - (image_real - (shift_real * guess_real + shift_imag * guess_imag)), source_imag - (image_imag - (shift_real * guess_imag - shift_imag * guess_real)))

def precondition(vector, diffusion, velocity):
    times = jnp.arange(L, dtype=jnp.float32)
    log_decay = math.log(alpha_corner) / L
    decay = math.exp(log_decay)
    scaled = vector * jnp.exp(times * log_decay)[:, None, None]
    spectrum = jnp.fft.fft(scaled, axis=0)
    source_real = jnp.real(spectrum)
    source_imag = jnp.imag(spectrum)
    angles = times * (2.0 * math.pi / L)
    shift_real = (decay * jnp.cos(angles))[:, None, None]
    shift_imag = (decay * jnp.sin(angles))[:, None, None]
    diag_real = 1.0 + 4.0 * diffusion - shift_real
    diag_imag = shift_imag
    modulus = diag_real * diag_real + diag_imag * diag_imag
    guess_real, guess_imag = divided(source_real, source_imag, diag_real, diag_imag, modulus)
    for sweep in range(SWEEPS - 1):
        image_real = apply_step(guess_real, diffusion, velocity)
        image_imag = apply_step(guess_imag, diffusion, velocity)
        left_real, left_imag = remainder(source_real, source_imag, image_real, image_imag, guess_real, guess_imag, shift_real, shift_imag)
        step_real, step_imag = divided(left_real, left_imag, diag_real, diag_imag, modulus)
        guess_real = guess_real + step_real
        guess_imag = guess_imag + step_imag
    back = jnp.real(jnp.fft.ifft(guess_real + 1j * guess_imag, axis=0))
    return back * jnp.exp(-times * log_decay)[:, None, None]

def least_squares(hessen, beta):
    ortho = []
    upper = [[None] * KRYLOV for row in range(KRYLOV)]
    for column in range(KRYLOV):
        current = hessen[:, column]
        for row in range(column):
            factor = jnp.sum(ortho[row] * current)
            upper[row][column] = factor
            current = current - factor * ortho[row]
        length = jnp.sqrt(jnp.sum(current * current))
        upper[column][column] = length
        ortho.append(current / length)
    target = [ortho[row][0] * beta for row in range(KRYLOV)]
    values = [None] * KRYLOV
    for row in reversed(range(KRYLOV)):
        accum = target[row]
        for later in range(row + 1, KRYLOV):
            accum = accum - upper[row][later] * values[later]
        values[row] = accum / upper[row][row]
    return jnp.stack(values)

def reference(right_side, diffusion, velocity):
    beta = jnp.sqrt(jnp.sum(right_side * right_side) + epsilon)
    basis = [right_side / beta]
    prepared = []
    hessen = jnp.zeros((KRYLOV + 1, KRYLOV), right_side.dtype)
    for column in range(KRYLOV):
        direction = precondition(basis[column], diffusion, velocity)
        prepared.append(direction)
        image = system(direction, diffusion, velocity)
        projections = jnp.stack([jnp.sum(vector * image) for vector in basis])
        for row in range(column + 1):
            image = image - projections[row] * basis[row]
        length = jnp.sqrt(jnp.sum(image * image) + epsilon)
        hessen = hessen.at[:column + 1, column].set(projections)
        hessen = hessen.at[column + 1, column].set(length)
        basis.append(image / length)
    coeffs = least_squares(hessen, beta)
    solution = prepared[0] * coeffs[0]
    for column in range(1, KRYLOV):
        solution = solution + prepared[column] * coeffs[column]
    first = (jnp.arange(KRYLOV + 1) == 0).astype(right_side.dtype)
    target = beta * first - lax.optimization_barrier(jnp.sum(hessen * coeffs[None, :], axis=1))
    residual = basis[0] * target[0]
    for row in range(1, KRYLOV + 1):
        residual = residual + basis[row] * target[row]
    return (solution, residual)
```

```python
import math

import jax
import jax.numpy as jnp
import numpy as np
from jax import lax
from jax.experimental import pallas as pl
from jax.experimental.pallas import tpu as pltpu
from jax.sharding import PartitionSpec as P

L = 512
KRYLOV = 3
ALPHA = 0.05
DAMPING = 0.8
EPSILON = 1e-06
LOG_DECAY = math.log(ALPHA) / L
DECAY = math.exp(LOG_DECAY)
MESH = pl.DeviceIdType.MESH
HIGHEST = lax.Precision.HIGHEST
F32 = jnp.float32


def tables():
    n = np.arange(L)
    k = np.arange(L // 2)
    angle = 2.0 * np.pi * ((n[:, None] * k[None, :]) % L) / L
    real = np.cos(angle)
    imag = -np.sin(angle)
    imag[:, 0] = np.where(n % 2 == 0, 1.0, -1.0)
    packed = np.concatenate([real, imag], axis=1)
    scale = np.full(L, 2.0 / L)
    scale[0] = scale[L // 2] = 1.0 / L
    decays = DECAY ** n
    forward = packed * decays[:, None]
    inverse = (packed * scale[None, :]).T / decays[None, :]
    shift_real = DECAY * np.cos(2.0 * np.pi * k / L)
    shift_imag = DECAY * np.sin(2.0 * np.pi * k / L)
    shift_other = shift_real.copy()
    shift_other[0] = -DECAY
    shift_imag[0] = 0.0
    corner = np.concatenate([shift_real * scale[: L // 2], shift_imag * scale[L // 2 :]])
    corner[L // 2] = -DECAY / L
    rows = np.concatenate([shift_real, shift_other, shift_imag, corner]).reshape(10, 128)
    small = np.zeros((16, 128))
    small[:10] = rows
    return forward.astype(np.float32), inverse.astype(np.float32), small.astype(np.float32)


def two_sum(a, b):
    s = a + b
    t = s - a
    return s, (a - (s - t)) + (b - t)


def split(a):
    c = 4097.0 * a
    high = c - (c - a)
    return high, a - high


def two_prod(a, b):
    p = a * b
    ah, al = split(a)
    bh, bl = split(b)
    return p, ((ah * bh - p) + ah * bl + al * bh) + al * bl


def pair_div(a, b):
    safe = jnp.where(b[0] > 0.0, b[0], 1.0)
    q = jnp.where(b[0] > 0.0, a[0] / safe, 0.0)
    p, e = two_prod(q, b[0])
    rest = ((a[0] - p) - e) + (a[1] - q * b[1])
    r = jnp.where(b[0] > 0.0, rest / safe, 0.0)
    s = q + r
    return s, r - (s - q)


def pair_less(a, m, b):
    p, e = two_prod(m[0], b[0])
    e = e + (m[0] * b[1] + m[1] * b[0])
    s, t = two_sum(a[0], -p)
    t = t + (a[1] - e)
    h = s + t
    return h, t - (h - s)


def krylov_weights(gram):
    n = KRYLOV + 1
    lower = [[None] * n for _ in range(n)]
    norm = [None] * n
    cross = [[None] * n for _ in range(n)]
    for k in range(n):
        for i in range(k, n):
            value = gram[k][i]
            for m in range(k):
                value = pair_less(value, lower[i][m], cross[k][m])
            cross[i][k] = value
        head = cross[k][k]
        keep = head[0] > 0.0
        head = (jnp.where(keep, head[0], 0.0), jnp.where(keep, head[1], 0.0))
        norm[k] = head[0]
        for i in range(k + 1, n):
            lower[i][k] = pair_div(cross[i][k], head)
    low = [[None if v is None else v[0] for v in row] for row in lower]
    zero = jnp.zeros_like(norm[0])
    images = []
    for k in range(KRYLOV):
        image = [low[k + 1][i] for i in range(k + 1)] + [zero + 1.0]
        for m in range(k):
            for i in range(m + 2):
                image[i] = image[i] - low[k][m] * images[m][i]
        images.append(image)
    beta = jnp.sqrt(norm[0] + EPSILON)
    basis = [[1.0 / beta]]
    hessen = [[zero] * KRYLOV for _ in range(n)]
    for j in range(KRYLOV):
        work = [zero] * (j + 2)
        for k in range(j + 1):
            for i in range(k + 2):
                work[i] = work[i] + basis[j][k] * images[k][i]
        for i in range(j + 1):
            total = zero
            for k in range(i + 1):
                total = total + basis[i][k] * norm[k] * work[k]
            hessen[i][j] = total
        for i in range(j + 1):
            for k in range(i + 1):
                work[k] = work[k] - hessen[i][j] * basis[i][k]
        total = zero
        for k in range(j + 2):
            total = total + work[k] * work[k] * norm[k]
        length = jnp.sqrt(total + EPSILON)
        hessen[j + 1][j] = length
        basis.append([v / length for v in work])
    ortho = []
    upper = [[None] * KRYLOV for _ in range(KRYLOV)]
    for column in range(KRYLOV):
        current = [hessen[i][column] for i in range(n)]
        for row in range(column):
            factor = sum(ortho[row][i] * current[i] for i in range(n))
            upper[row][column] = factor
            current = [current[i] - factor * ortho[row][i] for i in range(n)]
        length = jnp.sqrt(sum(v * v for v in current))
        upper[column][column] = length
        ortho.append([v / length for v in current])
    values = [None] * KRYLOV
    for row in reversed(range(KRYLOV)):
        accum = ortho[row][0] * beta
        for later in range(row + 1, KRYLOV):
            accum = accum - upper[row][later] * values[later]
        values[row] = accum / upper[row][row]
    target = []
    for i in range(n):
        accum = beta if i == 0 else zero
        for j in range(KRYLOV):
            accum = accum - hessen[i][j] * values[j]
        target.append(accum)

    def on_p(weights):
        on_u = [zero] * len(weights)
        for j, weight in enumerate(weights):
            for k in range(len(basis[j])):
                if k < len(weights):
                    on_u[k] = on_u[k] + weight * basis[j][k]
        for k in reversed(range(len(weights))):
            for i in range(k):
                on_u[i] = on_u[i] - low[k][i] * on_u[k]
        return on_u

    return on_p(values), on_p(target)


def lanes_below(count, shape=(8, 128)):
    return lax.broadcasted_iota(jnp.int32, shape, len(shape) - 1) < count


def lane_block(index):
    lane = lax.broadcasted_iota(jnp.int32, (8, 128), 1)
    return (lane >= 32 * index) & (lane < 32 * index + 32)


def turn(value, amount):
    amount = amount % 128
    return value if amount == 0 else pltpu.roll(value, amount, 1)


def kernel(
    b_ref, diff_ref, vel_ref, small_ref, fwd_hbm, inv_hbm,
    sol_ref, res_ref,
    fwd, inv,
    m1, r1, buf1, m2, r2, cd, cv, point, lead, own, edge4, edge2, h,
    left1, right1, left2, right2, north, south, nw, ne, sw, se, wa, wb,
    ar0, ar1, ar2, ars0, ars1, ars2, m3, r3, buf2, m4, r4,
    const_sem, coef_s, coef_r, s1_s, s1_r, s2_s, s2_r, ha_s, ha_r, a0_s, a0_r, a1_s, a1_r, a2_s, a2_r,
    s3_s, s3_r, s4_s, s4_r,
):
    tm = lax.axis_index("tm")
    x = lax.axis_index("space")
    z = tm // 16
    e_me = tm % 16
    y = e_me // 2
    core = e_me % 2
    odd = z % 2
    ys = y + odd * (7 - 2 * y)
    g = (z * 8 + ys) * 2 + core

    def at_strip(index):
        index = (index + 128) % 128
        strip = index // 2
        zz = strip // 8
        yy = strip % 8
        yy = yy + (zz % 2) * (7 - 2 * yy)
        return zz * 16 + yy * 2 + index % 2

    def place(t, s):
        return {"tm": t, "space": s}

    up = (x + 3) % 4
    down = (x + 1) % 4
    consts = [
        pltpu.make_async_copy(fwd_hbm, fwd, const_sem.at[0]),
        pltpu.make_async_copy(inv_hbm, inv, const_sem.at[1]),
    ]
    for copy in consts:
        copy.start()

    barrier = pltpu.get_barrier_semaphore()
    greet = [place(((z + d) % 8) * 16 + e_me, x) for d in range(1, 8)]
    greet += [place(z * 16 + (e_me + d) % 16, x) for d in range(1, 16)]
    greet += [place(tm, (x + d) % 4) for d in range(1, 4)]
    for d in (-2, -1, 1, 2):
        greet.append(place(at_strip(g + d), x))
    for d in (-1, 1):
        for s in (up, down):
            greet.append(place(at_strip(g + d), s))
    for device in greet:
        pl.semaphore_signal(barrier, inc=1, device_id=device, device_id_type=MESH)

    for zz in range(8):
        value = None
        for t in range(4):
            piece = turn(b_ref[t, :, (zz // 4) * 128 : (zz // 4) * 128 + 128], t * 32 - (zz % 4) * 32)
            value = piece if value is None else jnp.where(lane_block(t), piece, value)
        m1[zz] = value
    h[...] = jnp.zeros_like(h)
    wa[...] = jnp.zeros_like(wa)
    wb[...] = jnp.zeros_like(wb)
    r1[z] = m1[z]
    cd[1] = diff_ref[...]
    cv[1] = vel_ref[...]

    pl.semaphore_wait(barrier, len(greet))

    started = []

    def send(src, dst, s_sem, r_sem, device):
        copy = pltpu.make_async_remote_copy(
            src_ref=src, dst_ref=dst, send_sem=s_sem, recv_sem=r_sem, device_id=device, device_id_type=MESH
        )
        copy.start()
        started.append(copy)
        return copy

    stage1 = [
        send(m1.at[(z + d) % 8], r1.at[z], s1_s.at[d], s1_r.at[d], place(((z + d) % 8) * 16 + e_me, x))
        for d in range(1, 8)
    ]
    coefs = [
        send(diff_ref, cd.at[2], coef_s.at[0], coef_r.at[0], place(tm, up)),
        send(vel_ref, cv.at[2], coef_s.at[1], coef_r.at[1], place(tm, up)),
        send(diff_ref, cd.at[0], coef_s.at[2], coef_r.at[2], place(tm, down)),
        send(vel_ref, cv.at[0], coef_s.at[3], coef_r.at[3], place(tm, down)),
    ]
    for copy in stage1:
        copy.wait_recv()
    half = lanes_below(64, (16, 128))
    turned = jnp.transpose(r1[...].reshape(64, 128))
    buf1[:, 0:64] = turned
    for t in range(4):
        even = buf1[pl.ds(t * 32, 16, stride=2), :]
        other = buf1[pl.ds(t * 32 + 1, 16, stride=2), :]
        m2[:, t, :] = jnp.where(half, even, pltpu.roll(other, 64, 1))

    def strip_of(e):
        yy = e // 2
        return (yy + odd * (7 - 2 * yy)) * 2 + e % 2

    r2[e_me] = m2[strip_of(e_me)]
    stage2 = []
    for d in range(1, 16):
        to = (e_me + d) % 16
        stage2.append(
            send(m2.at[strip_of(to)], r2.at[e_me], s2_s.at[d], s2_r.at[d], place(z * 16 + to, x))
        )

    for copy in coefs:
        copy.wait_recv()
    parts = []
    for prev, mine, after in (
        (cd[0], cd[1], cd[2]),
        (cv[0, 0], cv[1, 0], cv[2, 0]),
        (cv[0, 1], cv[1, 1], cv[2, 1]),
    ):
        parts += [prev[4:8], mine, after[0:4]]
    stacked = jnp.concatenate(parts, axis=0)
    row_at = lax.broadcasted_iota(jnp.int32, (256, 128), 0)
    for j in range(8):
        pick = jnp.where(row_at == 2 * g - 3 + j, 1.0, 0.0).astype(F32)
        spread = jnp.dot(stacked, pick, precision=HIGHEST, preferred_element_type=F32)
        diff = spread[0:16]
        v_col = spread[16:32]
        v_row = spread[32:48]
        diag = 1.0 + 4.0 * diff
        point[0, j] = diag
        point[1, j] = -diff - v_row
        point[2, j] = -diff + v_row
        point[3, j] = -diff - v_col
        point[4, j] = -diff + v_col
        row = 8 * x - 4 + lax.broadcasted_iota(jnp.int32, (16, 128), 0)
        column = 2 * g - 3 + j
        inside = (row >= 0) & (row < 32) & (column >= 0) & (column < 256)
        for q in range(2):
            d_i = small_ref[4 + q : 5 + q, :]
            for which, base in ((0, 0), (1, 2)):
                d_r = diag - small_ref[base + q : base + q + 1, :]
                scale = jnp.where(inside, DAMPING / (d_r * d_r + d_i * d_i), 0.0)
                lead[which, q, j] = d_r * scale
                if which == 0:
                    lead[2, q, j] = d_i * scale

    for copy in stage2:
        copy.wait_recv()
    turned = jnp.transpose(r2[...].reshape(64, 128))
    low64 = lanes_below(64)
    tiles = []
    for cl in range(2):
        row = []
        for a in range(4):
            v0 = turned[cl * 64 + a * 16 : cl * 64 + a * 16 + 8, :]
            v1 = turned[cl * 64 + a * 16 + 8 : cl * 64 + a * 16 + 16, :]
            row.append(jnp.concatenate([v0, v1], axis=1))
        tiles.append(jnp.concatenate(row, axis=1))
    field = jnp.concatenate(tiles, axis=0)
    for copy in consts:
        copy.wait()
    spectrum = jnp.dot(field, fwd[...], precision=HIGHEST, preferred_element_type=F32)
    vectors = [field]
    directions = []

    def dot_pairs(a, b):
        high = low = None
        for cl in range(2):
            for q in range(4):
                va = a[cl * 8 : cl * 8 + 8, q * 128 : q * 128 + 128]
                vb = b[cl * 8 : cl * 8 + 8, q * 128 : q * 128 + 128]
                p, e = two_prod(va, vb)
                if high is None:
                    high, low = p, e
                else:
                    high, t = two_sum(high, p)
                    low = low + (t + e)
        for shift in (4, 2, 1):
            high, t = two_sum(high, pltpu.roll(high, shift, 0))
            low = low + pltpu.roll(low, shift, 0) + t
        return high, low

    grams = {}

    def put_spectrum(it, value):
        for q in range(4):
            for cl in range(2):
                own[it, q, cl] = value[cl * 8 : cl * 8 + 8, q * 128 : q * 128 + 128]
                edge4[it, 0, q, cl] = value[cl * 8 : cl * 8 + 4, q * 128 : q * 128 + 128]
                edge4[it, 1, q, cl] = value[cl * 8 + 4 : cl * 8 + 8, q * 128 : q * 128 + 128]
                edge2[it, 0, q, cl] = value[cl * 8 : cl * 8 + 2, q * 128 : q * 128 + 128]
                edge2[it, 1, q, cl] = value[cl * 8 + 6 : cl * 8 + 8, q * 128 : q * 128 + 128]

    def send_halo(it):
        n1, n2, p1, p2 = (at_strip(g - 1), at_strip(g - 2), at_strip(g + 1), at_strip(g + 2))
        moves = (
            (edge2.at[it, 1], nw.at[it], place(p1, down)),
            (edge2.at[it, 1], ne.at[it], place(n1, down)),
            (edge2.at[it, 0], sw.at[it], place(p1, up)),
            (edge2.at[it, 0], se.at[it], place(n1, up)),
            (own.at[it], left1.at[it], place(p1, x)),
            (own.at[it], right1.at[it], place(n1, x)),
            (edge4.at[it, 1], north.at[it], place(tm, down)),
            (edge4.at[it, 0], south.at[it], place(tm, up)),
            (own.at[it, :, 1], left2.at[it], place(p2, x)),
            (own.at[it, :, 0], right2.at[it], place(n2, x)),
        )
        return [
            send(src, dst, ha_s.at[it, i], ha_r.at[it, i], device)
            for i, (src, dst, device) in enumerate(moves)
        ]

    def shifts(q):
        return (small_ref[q : q + 1, :], small_ref[2 + q : 3 + q, :], small_ref[4 + q : 5 + q, :])

    def stencil(w, q, j, start, rows, at):
        here = w[q, j, pl.ds(start, rows), :]
        return here, (
            point[0, j, pl.ds(at, rows), :] * here
            + point[1, j, pl.ds(at, rows), :] * w[q, j, pl.ds(start - 1, rows), :]
            + point[2, j, pl.ds(at, rows), :] * w[q, j, pl.ds(start + 1, rows), :]
            + point[3, j, pl.ds(at, rows), :] * w[q, j - 1, pl.ds(start, rows), :]
            + point[4, j, pl.ds(at, rows), :] * w[q, j + 1, pl.ds(start, rows), :]
        )

    def sweep(source, target, first, last):
        def body(j, carry):
            for at in (0, 8):
                for q in range(2):
                    s_re, s_im, s_x = shifts(q)
                    w_re, b_re = stencil(source, q, j, 8 + at, 8, at)
                    w_im, b_im = stencil(source, q + 2, j, 8 + at, 8, at)
                    rows = pl.ds(at, 8)
                    left_re = h[q, j, rows, :] - (b_re - (s_re * w_re + s_x * w_im))
                    left_im = h[q + 2, j, rows, :] - (b_im - (s_im * w_im - s_x * w_re))
                    p_re, p_im, p_x = lead[0, q, j, rows, :], lead[1, q, j, rows, :], lead[2, q, j, rows, :]
                    target[q, j, pl.ds(8 + at, 8), :] = w_re + (p_re * left_re + p_x * left_im)
                    target[q + 2, j, pl.ds(8 + at, 8), :] = w_im + (p_im * left_im - p_x * left_re)
            return carry

        lax.fori_loop(first, last, body, 0)

    put_spectrum(0, spectrum)
    halo = send_halo(0)
    grams[0, 0] = dot_pairs(field, field)

    for it in range(KRYLOV):
        for q in range(4):
            for cl in range(2):
                h[q, 3 + cl, 4:12, :] = own[it, q, cl]
        for copy in halo:
            copy.wait_recv()
        for q in range(4):
            h[q, 0, 4:12, :] = left2[it, q]
            h[q, 7, 4:12, :] = right2[it, q]
            for cl in range(2):
                h[q, 1 + cl, 4:12, :] = left1[it, q, cl]
                h[q, 1 + cl, 2:4, :] = nw[it, q, cl]
                h[q, 1 + cl, 12:14, :] = sw[it, q, cl]
                h[q, 5 + cl, 4:12, :] = right1[it, q, cl]
                h[q, 5 + cl, 2:4, :] = ne[it, q, cl]
                h[q, 5 + cl, 12:14, :] = se[it, q, cl]
                h[q, 3 + cl, 0:4, :] = north[it, q, cl]
                h[q, 3 + cl, 12:16, :] = south[it, q, cl]

        def first_guess(j, carry):
            for at in (0, 8):
                rows = pl.ds(at, 8)
                for q in range(2):
                    re, im = h[q, j, rows, :], h[q + 2, j, rows, :]
                    p_re, p_im, p_x = lead[0, q, j, rows, :], lead[1, q, j, rows, :], lead[2, q, j, rows, :]
                    wa[q, j, pl.ds(8 + at, 8), :] = p_re * re + p_x * im
                    wa[q + 2, j, pl.ds(8 + at, 8), :] = p_im * im - p_x * re
            return carry

        lax.fori_loop(0, 8, first_guess, 0)
        sweep(wa, wb, 1, 7)
        sweep(wb, wa, 2, 6)
        guess, image = [], []
        for cl in range(2):
            j = 3 + cl
            w_row, g_row = [None] * 4, [None] * 4
            for q in range(2):
                s_re, s_im, s_x = shifts(q)
                w_re, b_re = stencil(wa, q, j, 12, 8, 4)
                w_im, b_im = stencil(wa, q + 2, j, 12, 8, 4)
                w_row[q], w_row[q + 2] = w_re, w_im
                g_row[q] = b_re - (s_re * w_re + s_x * w_im)
                g_row[q + 2] = b_im - (s_im * w_im - s_x * w_re)
            mean = w_row[0] * small_ref[6:7, :]
            for q in range(1, 4):
                mean = mean + w_row[q] * small_ref[6 + q : 7 + q, :]
            corner = jnp.broadcast_to(jnp.sum(mean, axis=1, keepdims=True), (8, 128))
            g_row[0] = g_row[0] + corner
            g_row[1] = g_row[1] + corner
            g_row[2] = g_row[2] + jnp.where(lanes_below(1), corner, 0.0)
            guess.append(jnp.concatenate(w_row, axis=1))
            image.append(jnp.concatenate(g_row, axis=1))
        guess = jnp.concatenate(guess, axis=0)
        image = jnp.concatenate(image, axis=0)
        if it + 1 < KRYLOV:
            put_spectrum(it + 1, image)
            halo = send_halo(it + 1)
        both = jnp.dot(
            jnp.concatenate([guess, image], axis=0), inv[...], precision=HIGHEST, preferred_element_type=F32
        )
        directions.append(both[0:16])
        vectors.append(both[16:32])
        for i in range(it + 2):
            grams[i, it + 1] = dot_pairs(vectors[i], vectors[it + 1])

    order = [(i, j) for i in range(KRYLOV + 1) for j in range(i, KRYLOV + 1)]
    row_is = lax.broadcasted_iota(jnp.int32, (16, 128), 0)
    lane_is = lax.broadcasted_iota(jnp.int32, (16, 128), 1)
    high = jnp.zeros((16, 128), F32)
    low = jnp.zeros((16, 128), F32)
    for n, key in enumerate(order):
        a, b = grams[key]
        high = jnp.where(row_is == n, jnp.concatenate([a, a], axis=0), high)
        low = jnp.where(row_is == n, jnp.concatenate([b, b], axis=0), low)
    for shift in (64, 32, 16, 8, 4, 2, 1):
        high, t = two_sum(high, pltpu.roll(high, shift, 1))
        low = low + pltpu.roll(low, shift, 1) + t
    packed = jnp.where(lane_is == row_is, high, jnp.where(lane_is == row_is + 16, low, 0.0))
    mine = jnp.sum(packed, axis=0, keepdims=True)

    def all_add(mine, src, dst, s_sem, r_sem, devices, me):
        count = len(devices) + 1
        src[...] = mine
        dst[me] = mine
        copies = [
            send(src, dst.at[me], s_sem.at[d], r_sem.at[d], device)
            for d, device in enumerate(devices, start=1)
        ]
        for copy in copies:
            copy.wait_recv()
        level = [(dst[i], None) for i in range(count)]
        while len(level) > 1:
            following = []
            for (a, ea), (b, eb) in zip(level[::2], level[1::2]):
                s, t = two_sum(a, b)
                for extra in (ea, eb):
                    t = t if extra is None else t + extra
                following.append((s, t))
            level = following
        s, t = level[0]
        lane = lax.broadcasted_iota(jnp.int32, (1, 128), 1)
        return s + jnp.where((lane >= 16) & (lane < 32), pltpu.roll(t, 16, 1), 0.0)

    mine = all_add(
        mine, ars0, ar0, a0_s, a0_r, [place(z * 16 + (e_me + d) % 16, x) for d in range(1, 16)], e_me
    )
    mine = all_add(
        mine, ars1, ar1, a1_s, a1_r, [place(((z + d) % 8) * 16 + e_me, x) for d in range(1, 8)], z
    )
    mine = all_add(mine, ars2, ar2, a2_s, a2_r, [place(tm, (x + d) % 4) for d in range(1, 4)], x)
    mine = jnp.broadcast_to(mine, (8, 128))
    gram = [[None] * (KRYLOV + 1) for _ in range(KRYLOV + 1)]
    for n, (i, j) in enumerate(order):
        value = (
            jnp.broadcast_to(mine[:, n : n + 1], (8, 128)),
            jnp.broadcast_to(mine[:, 16 + n : 17 + n], (8, 128)),
        )
        gram[i][j] = value
        gram[j][i] = value
    on_directions, on_vectors = krylov_weights(gram)

    def combined(weights, fields, cl, q):
        total = None
        for weight, value in zip(weights, fields):
            term = weight * value[cl * 8 : cl * 8 + 8, q * 128 : q * 128 + 128]
            total = term if total is None else total + term
        return total

    rows = []
    for cl in range(2):
        for a in range(4):
            f0 = combined(on_directions, directions, cl, a)
            f1 = combined(on_vectors, vectors, cl, a)
            rows.append(jnp.where(low64, f0, pltpu.roll(f1, 64, 1)))
            rows.append(jnp.where(low64, pltpu.roll(f0, 64, 1), f1))
    turned = jnp.transpose(jnp.concatenate(rows, axis=0))
    for src in range(16):
        for f in range(2):
            m3[src, f * 4 : f * 4 + 4, :] = turned[f * 64 + src * 4 : f * 64 + src * 4 + 4, :]
    strip_me = strip_of(e_me)
    r3[strip_me] = m3[e_me]
    stage3 = []
    for d in range(1, 16):
        to = (e_me + d) % 16
        stage3.append(send(m3.at[to], r3.at[strip_me], s3_s.at[d], s3_r.at[d], place(z * 16 + to, x)))
    for copy in stage3:
        copy.wait_recv()
    for t in range(4):
        f0 = r3[:, t, :]
        f1 = r3[:, 4 + t, :]
        buf2[pl.ds(t * 32, 16, stride=2), :] = jnp.where(half, f0, pltpu.roll(f1, 64, 1))
        buf2[pl.ds(t * 32 + 1, 16, stride=2), :] = jnp.where(half, pltpu.roll(f0, 64, 1), f1)
    turned = jnp.transpose(buf2[...])
    for zz in range(8):
        for f in range(2):
            m4[zz, f] = turned[f * 64 + zz * 8 : f * 64 + zz * 8 + 8, :]
    r4[z] = m4[z]
    stage4 = [
        send(m4.at[(z + d) % 8], r4.at[z], s4_s.at[d], s4_r.at[d], place(((z + d) % 8) * 16 + e_me, x))
        for d in range(1, 8)
    ]
    for copy in stage4:
        copy.wait_recv()
    for f, out in ((0, sol_ref), (1, res_ref)):
        for t in range(4):
            for hh in range(2):
                value = None
                for k in range(4):
                    piece = turn(r4[hh * 4 + k, f], k * 32 - t * 32)
                    value = piece if value is None else jnp.where(lane_block(k), piece, value)
                out[t, :, hh * 128 : hh * 128 + 128] = value
    for copy in started:
        copy.wait_send()


def per_device(right_side, diffusion, velocity):
    forward, inverse, small = tables()
    vmem = pl.BlockSpec(memory_space=pltpu.VMEM)
    anywhere = pl.BlockSpec(memory_space=pl.ANY)

    def buffer(*shape):
        return pltpu.VMEM(shape, F32)

    def sems(*shape):
        return pltpu.SemaphoreType.DMA(shape)

    out = jax.ShapeDtypeStruct(right_side.shape, F32)
    return pl.pallas_call(
        kernel,
        out_shape=(out, out),
        in_specs=[vmem, vmem, vmem, vmem, anywhere, anywhere],
        out_specs=(vmem, vmem),
        scratch_shapes=[
            buffer(L, L), buffer(L, L),
            buffer(8, 8, 128), buffer(8, 8, 128), buffer(128, 128), buffer(16, 4, 128), buffer(16, 4, 128),
            buffer(3, 8, 256), buffer(3, 2, 8, 256),
            buffer(5, 8, 16, 128), buffer(3, 2, 8, 16, 128),
            buffer(3, 4, 2, 8, 128), buffer(3, 2, 4, 2, 4, 128), buffer(3, 2, 4, 2, 2, 128),
            buffer(4, 8, 16, 128),
            buffer(3, 4, 2, 8, 128), buffer(3, 4, 2, 8, 128), buffer(3, 4, 8, 128), buffer(3, 4, 8, 128),
            buffer(3, 4, 2, 4, 128), buffer(3, 4, 2, 4, 128),
            buffer(3, 4, 2, 2, 128), buffer(3, 4, 2, 2, 128), buffer(3, 4, 2, 2, 128), buffer(3, 4, 2, 2, 128),
            buffer(4, 8, 32, 128), buffer(4, 8, 32, 128),
            buffer(16, 1, 128), buffer(8, 1, 128), buffer(4, 1, 128),
            buffer(1, 128), buffer(1, 128), buffer(1, 128),
            buffer(16, 8, 128), buffer(16, 8, 128), buffer(128, 128),
            buffer(8, 2, 8, 128), buffer(8, 2, 8, 128),
            sems(2), sems(4), sems(4), sems(8), sems(8), sems(16), sems(16), sems(3, 10), sems(3, 10),
            sems(16), sems(16), sems(8), sems(8), sems(4), sems(4), sems(16), sems(16), sems(8), sems(8),
        ],
        compiler_params=pltpu.CompilerParams(
            collective_id=0, has_side_effects=True, vmem_limit_bytes=32 * 1024 * 1024
        ),
    )(right_side, diffusion, velocity, small, forward, inverse)


def solution(mesh):
    return jax.shard_map(
        per_device,
        mesh=mesh,
        in_specs=(P("tm", "space", None), P("space", None), P(None, "space", None)),
        out_specs=(P("tm", "space", None), P("tm", "space", None)),
        check_vma=False,
    )
```

```python
import math

import jax
import jax.numpy as jnp
import numpy as np
from jax import lax
from jax.experimental import pallas as pl
from jax.experimental.pallas import tpu as pltpu
from jax.sharding import PartitionSpec as P

L = 512
KRYLOV = 3
ALPHA = 0.05
DAMPING = 0.8
EPSILON = 1e-06
LOG_DECAY = math.log(ALPHA) / L
DECAY = math.exp(LOG_DECAY)
MESH = pl.DeviceIdType.MESH
HIGHEST = lax.Precision.HIGHEST
FAR_8 = (4, 3, 5, 2, 6, 1, 7)
FAR_16 = (8, 7, 9, 6, 10, 5, 11, 4, 12, 3, 13, 2, 14, 1, 15)
F32 = jnp.float32


def tables():
    n = np.arange(L)
    k = np.arange(L // 2)
    angle = 2.0 * np.pi * ((n[:, None] * k[None, :]) % L) / L
    real = np.cos(angle)
    imag = -np.sin(angle)
    imag[:, 0] = np.where(n % 2 == 0, 1.0, -1.0)
    packed = np.concatenate([real, imag], axis=1)
    scale = np.full(L, 2.0 / L)
    scale[0] = scale[L // 2] = 1.0 / L
    decays = DECAY ** n
    forward = packed * decays[:, None]
    inverse = (packed * scale[None, :]).T / decays[None, :]
    shift_real = DECAY * np.cos(2.0 * np.pi * k / L)
    shift_imag = DECAY * np.sin(2.0 * np.pi * k / L)
    shift_other = shift_real.copy()
    shift_other[0] = -DECAY
    shift_imag[0] = 0.0
    corner = np.concatenate([shift_real * scale[: L // 2], shift_imag * scale[L // 2 :]])
    corner[L // 2] = -DECAY / L
    rows = np.concatenate([shift_real, shift_other, shift_imag, corner]).reshape(10, 128)
    small = np.zeros((16, 128))
    small[:10] = rows
    return forward.astype(np.float32), inverse.astype(np.float32), small.astype(np.float32)


def two_sum(a, b):
    s = a + b
    t = s - a
    return s, (a - (s - t)) + (b - t)


def split(a):
    c = 4097.0 * a
    high = c - (c - a)
    return high, a - high


def two_prod(a, b):
    p = a * b
    ah, al = split(a)
    bh, bl = split(b)
    return p, ((ah * bh - p) + ah * bl + al * bh) + al * bl


def pair_div(a, b):
    safe = jnp.where(b[0] > 0.0, b[0], 1.0)
    q = jnp.where(b[0] > 0.0, a[0] / safe, 0.0)
    p, e = two_prod(q, b[0])
    rest = ((a[0] - p) - e) + (a[1] - q * b[1])
    r = jnp.where(b[0] > 0.0, rest / safe, 0.0)
    s = q + r
    return s, r - (s - q)


def pair_less(a, m, b):
    p, e = two_prod(m[0], b[0])
    e = e + (m[0] * b[1] + m[1] * b[0])
    s, t = two_sum(a[0], -p)
    t = t + (a[1] - e)
    h = s + t
    return h, t - (h - s)


def krylov_weights(gram):
    n = KRYLOV + 1
    lower = [[None] * n for _ in range(n)]
    norm = [None] * n
    cross = [[None] * n for _ in range(n)]
    for k in range(n):
        for i in range(k, n):
            value = gram[k][i]
            for m in range(k):
                value = pair_less(value, lower[i][m], cross[k][m])
            cross[i][k] = value
        head = cross[k][k]
        keep = head[0] > 0.0
        head = (jnp.where(keep, head[0], 0.0), jnp.where(keep, head[1], 0.0))
        norm[k] = head[0]
        for i in range(k + 1, n):
            lower[i][k] = pair_div(cross[i][k], head)
    low = [[None if v is None else v[0] for v in row] for row in lower]
    zero = jnp.zeros_like(norm[0])
    images = []
    for k in range(KRYLOV):
        image = [low[k + 1][i] for i in range(k + 1)] + [zero + 1.0]
        for m in range(k):
            for i in range(m + 2):
                image[i] = image[i] - low[k][m] * images[m][i]
        images.append(image)
    beta = jnp.sqrt(norm[0] + EPSILON)
    basis = [[1.0 / beta]]
    hessen = [[zero] * KRYLOV for _ in range(n)]
    for j in range(KRYLOV):
        work = [zero] * (j + 2)
        for k in range(j + 1):
            for i in range(k + 2):
                work[i] = work[i] + basis[j][k] * images[k][i]
        for i in range(j + 1):
            total = zero
            for k in range(i + 1):
                total = total + basis[i][k] * norm[k] * work[k]
            hessen[i][j] = total
        for i in range(j + 1):
            for k in range(i + 1):
                work[k] = work[k] - hessen[i][j] * basis[i][k]
        total = zero
        for k in range(j + 2):
            total = total + work[k] * work[k] * norm[k]
        length = jnp.sqrt(total + EPSILON)
        hessen[j + 1][j] = length
        basis.append([v / length for v in work])
    ortho = []
    upper = [[None] * KRYLOV for _ in range(KRYLOV)]
    for column in range(KRYLOV):
        current = [hessen[i][column] for i in range(n)]
        for row in range(column):
            factor = sum(ortho[row][i] * current[i] for i in range(n))
            upper[row][column] = factor
            current = [current[i] - factor * ortho[row][i] for i in range(n)]
        length = jnp.sqrt(sum(v * v for v in current))
        upper[column][column] = length
        ortho.append([v / length for v in current])
    values = [None] * KRYLOV
    for row in reversed(range(KRYLOV)):
        accum = ortho[row][0] * beta
        for later in range(row + 1, KRYLOV):
            accum = accum - upper[row][later] * values[later]
        values[row] = accum / upper[row][row]
    target = []
    for i in range(n):
        accum = beta if i == 0 else zero
        for j in range(KRYLOV):
            accum = accum - hessen[i][j] * values[j]
        target.append(accum)

    def on_p(weights):
        on_u = [zero] * len(weights)
        for j, weight in enumerate(weights):
            for k in range(len(basis[j])):
                if k < len(weights):
                    on_u[k] = on_u[k] + weight * basis[j][k]
        for k in reversed(range(len(weights))):
            for i in range(k):
                on_u[i] = on_u[i] - low[k][i] * on_u[k]
        return on_u

    return on_p(values), on_p(target)


def lanes_below(count, shape=(8, 128)):
    return lax.broadcasted_iota(jnp.int32, shape, len(shape) - 1) < count


def lane_block(index):
    lane = lax.broadcasted_iota(jnp.int32, (8, 128), 1)
    return (lane >= 32 * index) & (lane < 32 * index + 32)


def turn(value, amount):
    amount = amount % 128
    return value if amount == 0 else pltpu.roll(value, amount, 1)


def kernel(
    b_hbm, diff_hbm, vel_hbm, small_hbm, fwd_hbm, inv_hbm,
    sol_ref, res_ref,
    b_ref, diff_ref, vel_ref, small_ref, fwd, inv,
    m1, r1, buf1, m2, r2, cd, cv, point, lead, own, edge4, edge2, h,
    left1, right1, left2, right2, north, south, nw, ne, sw, se, wa, wb,
    ar0, ar1, ar2, ars0, ars1, ars2, m3, r3, buf2, m4, r4,
    const_sem, coef_s, coef_r, s1_s, s1_r, s2_s, s2_r, ha_s, ha_r, a0_s, a0_r, a1_s, a1_r, a2_s, a2_r,
    s3_s, s3_r, s4_s, s4_r,
):
    tm = lax.axis_index("tm")
    x = lax.axis_index("space")
    z = tm // 16
    e_me = tm % 16
    y = e_me // 2
    core = e_me % 2
    odd = z % 2
    ys = y + odd * (7 - 2 * y)
    g = (z * 8 + ys) * 2 + core

    def at_strip(index):
        index = (index + 128) % 128
        strip = index // 2
        zz = strip // 8
        yy = strip % 8
        yy = yy + (zz % 2) * (7 - 2 * yy)
        return zz * 16 + yy * 2 + index % 2

    def place(t, s):
        return {"tm": t, "space": s}

    up = (x + 3) % 4
    down = (x + 1) % 4
    loads = [
        pltpu.make_async_copy(src, dst, const_sem.at[i])
        for i, (src, dst) in enumerate(
            (
                (b_hbm, b_ref), (diff_hbm, diff_ref), (vel_hbm, vel_ref),
                (small_hbm, small_ref), (fwd_hbm, fwd), (inv_hbm, inv),
            )
        )
    ]
    loads[0].start()
    barrier = pltpu.get_barrier_semaphore()
    greet = [place(((z + d) % 8) * 16 + e_me, x) for d in FAR_8]
    greet += [place(z * 16 + (e_me + d) % 16, x) for d in FAR_16]
    greet += [place(tm, (x + d) % 4) for d in range(1, 4)]
    for d in (-2, -1, 1, 2):
        greet.append(place(at_strip(g + d), x))
    for d in (-1, 1):
        for s in (up, down):
            greet.append(place(at_strip(g + d), s))
    for device in greet:
        pl.semaphore_signal(barrier, inc=1, device_id=device, device_id_type=MESH)
    for copy in loads[1:]:
        copy.start()
    loads[0].wait()

    for zz in range(8):
        value = None
        for t in range(4):
            piece = turn(b_ref[t, :, (zz // 4) * 128 : (zz // 4) * 128 + 128], t * 32 - (zz % 4) * 32)
            value = piece if value is None else jnp.where(lane_block(t), piece, value)
        m1[zz] = value
    r1[z] = m1[z]
    loads[1].wait()
    loads[2].wait()

    pl.semaphore_wait(barrier, len(greet))

    started = []

    def send(src, dst, s_sem, r_sem, device):
        copy = pltpu.make_async_remote_copy(
            src_ref=src, dst_ref=dst, send_sem=s_sem, recv_sem=r_sem, device_id=device, device_id_type=MESH
        )
        copy.start()
        started.append(copy)
        return copy

    stage1 = [
        send(m1.at[(z + d) % 8], r1.at[z], s1_s.at[d], s1_r.at[d], place(((z + d) % 8) * 16 + e_me, x))
        for d in FAR_8
    ]
    coefs = [
        send(diff_ref, cd.at[2], coef_s.at[0], coef_r.at[0], place(tm, up)),
        send(vel_ref, cv.at[2], coef_s.at[1], coef_r.at[1], place(tm, up)),
        send(diff_ref, cd.at[0], coef_s.at[2], coef_r.at[2], place(tm, down)),
        send(vel_ref, cv.at[0], coef_s.at[3], coef_r.at[3], place(tm, down)),
    ]
    h[...] = jnp.zeros_like(h)
    wa[...] = jnp.zeros_like(wa)
    wb[...] = jnp.zeros_like(wb)
    cd[1] = diff_ref[...]
    cv[1] = vel_ref[...]
    loads[3].wait()
    for copy in stage1:
        copy.wait_recv()
    half = lanes_below(64, (16, 128))
    turned = jnp.transpose(r1[...].reshape(64, 128))
    buf1[:, 0:64] = turned
    for t in range(4):
        even = buf1[pl.ds(t * 32, 16, stride=2), :]
        other = buf1[pl.ds(t * 32 + 1, 16, stride=2), :]
        m2[:, t, :] = jnp.where(half, even, pltpu.roll(other, 64, 1))

    def strip_of(e):
        yy = e // 2
        return (yy + odd * (7 - 2 * yy)) * 2 + e % 2

    r2[e_me] = m2[strip_of(e_me)]
    stage2 = []
    for d in FAR_16:
        to = (e_me + d) % 16
        stage2.append(
            send(m2.at[strip_of(to)], r2.at[e_me], s2_s.at[d], s2_r.at[d], place(z * 16 + to, x))
        )

    for copy in coefs:
        copy.wait_recv()
    parts = []
    for prev, mine, after in (
        (cd[0], cd[1], cd[2]),
        (cv[0, 0], cv[1, 0], cv[2, 0]),
        (cv[0, 1], cv[1, 1], cv[2, 1]),
    ):
        parts += [prev[4:8], mine, after[0:4]]
    stacked = jnp.concatenate(parts, axis=0)
    row_at = lax.broadcasted_iota(jnp.int32, (256, 128), 0)
    for j in range(8):
        pick = jnp.where(row_at == 2 * g - 3 + j, 1.0, 0.0).astype(F32)
        spread = jnp.dot(stacked, pick, precision=HIGHEST, preferred_element_type=F32)
        diff = spread[0:16]
        v_col = spread[16:32]
        v_row = spread[32:48]
        diag = 1.0 + 4.0 * diff
        point[0, j] = diag
        point[1, j] = -diff - v_row
        point[2, j] = -diff + v_row
        point[3, j] = -diff - v_col
        point[4, j] = -diff + v_col
        row = 8 * x - 4 + lax.broadcasted_iota(jnp.int32, (16, 128), 0)
        column = 2 * g - 3 + j
        inside = (row >= 0) & (row < 32) & (column >= 0) & (column < 256)
        for q in range(2):
            d_i = small_ref[4 + q : 5 + q, :]
            for which, base in ((0, 0), (1, 2)):
                d_r = diag - small_ref[base + q : base + q + 1, :]
                scale = jnp.where(inside, DAMPING / (d_r * d_r + d_i * d_i), 0.0)
                lead[which, q, j] = d_r * scale
                if which == 0:
                    lead[2, q, j] = d_i * scale

    for copy in stage2:
        copy.wait_recv()
    turned = jnp.transpose(r2[...].reshape(64, 128))
    low64 = lanes_below(64)
    tiles = []
    for cl in range(2):
        row = []
        for a in range(4):
            v0 = turned[cl * 64 + a * 16 : cl * 64 + a * 16 + 8, :]
            v1 = turned[cl * 64 + a * 16 + 8 : cl * 64 + a * 16 + 16, :]
            row.append(jnp.concatenate([v0, v1], axis=1))
        tiles.append(jnp.concatenate(row, axis=1))
    field = jnp.concatenate(tiles, axis=0)
    loads[4].wait()
    loads[5].wait()
    spectrum = jnp.dot(field, fwd[...], precision=HIGHEST, preferred_element_type=F32)
    vectors = [field]
    directions = []

    def dot_pairs(a, b):
        high = low = None
        for cl in range(2):
            for q in range(4):
                va = a[cl * 8 : cl * 8 + 8, q * 128 : q * 128 + 128]
                vb = b[cl * 8 : cl * 8 + 8, q * 128 : q * 128 + 128]
                p, e = two_prod(va, vb)
                if high is None:
                    high, low = p, e
                else:
                    high, t = two_sum(high, p)
                    low = low + (t + e)
        for shift in (4, 2, 1):
            high, t = two_sum(high, pltpu.roll(high, shift, 0))
            low = low + pltpu.roll(low, shift, 0) + t
        return high, low

    grams = {}

    def put_spectrum(it, value):
        for q in range(4):
            for cl in range(2):
                own[it, q, cl] = value[cl * 8 : cl * 8 + 8, q * 128 : q * 128 + 128]
                edge4[it, 0, q, cl] = value[cl * 8 : cl * 8 + 4, q * 128 : q * 128 + 128]
                edge4[it, 1, q, cl] = value[cl * 8 + 4 : cl * 8 + 8, q * 128 : q * 128 + 128]
                edge2[it, 0, q, cl] = value[cl * 8 : cl * 8 + 2, q * 128 : q * 128 + 128]
                edge2[it, 1, q, cl] = value[cl * 8 + 6 : cl * 8 + 8, q * 128 : q * 128 + 128]

    def send_halo(it):
        n1, n2, p1, p2 = (at_strip(g - 1), at_strip(g - 2), at_strip(g + 1), at_strip(g + 2))
        moves = (
            (edge2.at[it, 1], nw.at[it], place(p1, down)),
            (edge2.at[it, 1], ne.at[it], place(n1, down)),
            (edge2.at[it, 0], sw.at[it], place(p1, up)),
            (edge2.at[it, 0], se.at[it], place(n1, up)),
            (own.at[it], left1.at[it], place(p1, x)),
            (own.at[it], right1.at[it], place(n1, x)),
            (edge4.at[it, 1], north.at[it], place(tm, down)),
            (edge4.at[it, 0], south.at[it], place(tm, up)),
            (own.at[it, :, 1], left2.at[it], place(p2, x)),
            (own.at[it, :, 0], right2.at[it], place(n2, x)),
        )
        return [
            send(src, dst, ha_s.at[it, i], ha_r.at[it, i], device)
            for i, (src, dst, device) in enumerate(moves)
        ]

    def shifts(q):
        return (small_ref[q : q + 1, :], small_ref[2 + q : 3 + q, :], small_ref[4 + q : 5 + q, :])

    def stencil(w, q, j, start, rows, at):
        here = w[q, j, pl.ds(start, rows), :]
        return here, (
            point[0, j, pl.ds(at, rows), :] * here
            + point[1, j, pl.ds(at, rows), :] * w[q, j, pl.ds(start - 1, rows), :]
            + point[2, j, pl.ds(at, rows), :] * w[q, j, pl.ds(start + 1, rows), :]
            + point[3, j, pl.ds(at, rows), :] * w[q, j - 1, pl.ds(start, rows), :]
            + point[4, j, pl.ds(at, rows), :] * w[q, j + 1, pl.ds(start, rows), :]
        )

    def sweep(source, target, first, last):
        def body(j, carry):
            for at in (0, 8):
                for q in range(2):
                    s_re, s_im, s_x = shifts(q)
                    w_re, b_re = stencil(source, q, j, 8 + at, 8, at)
                    w_im, b_im = stencil(source, q + 2, j, 8 + at, 8, at)
                    rows = pl.ds(at, 8)
                    left_re = h[q, j, rows, :] - (b_re - (s_re * w_re + s_x * w_im))
                    left_im = h[q + 2, j, rows, :] - (b_im - (s_im * w_im - s_x * w_re))
                    p_re, p_im, p_x = lead[0, q, j, rows, :], lead[1, q, j, rows, :], lead[2, q, j, rows, :]
                    target[q, j, pl.ds(8 + at, 8), :] = w_re + (p_re * left_re + p_x * left_im)
                    target[q + 2, j, pl.ds(8 + at, 8), :] = w_im + (p_im * left_im - p_x * left_re)
            return carry

        lax.fori_loop(first, last, body, 0)

    strip_me = strip_of(e_me)
    stage3, stage4 = {}, {}

    def pieces(value):
        return [[value[cl * 8 : cl * 8 + 8, q * 128 : q * 128 + 128] for q in range(4)] for cl in range(2)]

    def send_strip(it):
        p0, p1 = pieces(directions[it]), pieces(vectors[it + 1])
        rows = []
        for cl in range(2):
            for a in range(4):
                f0, f1 = p0[cl][a], p1[cl][a]
                rows.append(jnp.where(low64, f0, pltpu.roll(f1, 64, 1)))
                rows.append(jnp.where(low64, pltpu.roll(f0, 64, 1), f1))
        turned = jnp.transpose(jnp.concatenate(rows, axis=0))
        for src in range(16):
            for f in range(2):
                m3[it, src, f * 4 : f * 4 + 4, :] = turned[f * 64 + src * 4 : f * 64 + src * 4 + 4, :]
        r3[it, strip_me] = m3[it, e_me]
        stage3[it] = []
        for d in FAR_16:
            to = (e_me + d) % 16
            stage3[it].append(
                send(m3.at[it, to], r3.at[it, strip_me], s3_s.at[it, d], s3_r.at[it, d], place(z * 16 + to, x))
            )

    def send_steps(it):
        for copy in stage3[it]:
            copy.wait_recv()
        for t in range(4):
            f0 = r3[it, :, t, :]
            f1 = r3[it, :, 4 + t, :]
            buf2[pl.ds(t * 32, 16, stride=2), :] = jnp.where(half, f0, pltpu.roll(f1, 64, 1))
            buf2[pl.ds(t * 32 + 1, 16, stride=2), :] = jnp.where(half, pltpu.roll(f0, 64, 1), f1)
        turned = jnp.transpose(buf2[...])
        for zz in range(8):
            for f in range(2):
                m4[it, zz, f] = turned[f * 64 + zz * 8 : f * 64 + zz * 8 + 8, :]
        r4[it, z] = m4[it, z]
        stage4[it] = [
            send(
                m4.at[it, (z + d) % 8], r4.at[it, z], s4_s.at[it, d], s4_r.at[it, d],
                place(((z + d) % 8) * 16 + e_me, x),
            )
            for d in FAR_8
        ]

    put_spectrum(0, spectrum)
    halo = send_halo(0)
    grams[0, 0] = dot_pairs(field, field)

    for it in range(KRYLOV):
        for q in range(4):
            for cl in range(2):
                h[q, 3 + cl, 4:12, :] = own[it, q, cl]
        for copy in halo:
            copy.wait_recv()
        for q in range(4):
            h[q, 0, 4:12, :] = left2[it, q]
            h[q, 7, 4:12, :] = right2[it, q]
            for cl in range(2):
                h[q, 1 + cl, 4:12, :] = left1[it, q, cl]
                h[q, 1 + cl, 2:4, :] = nw[it, q, cl]
                h[q, 1 + cl, 12:14, :] = sw[it, q, cl]
                h[q, 5 + cl, 4:12, :] = right1[it, q, cl]
                h[q, 5 + cl, 2:4, :] = ne[it, q, cl]
                h[q, 5 + cl, 12:14, :] = se[it, q, cl]
                h[q, 3 + cl, 0:4, :] = north[it, q, cl]
                h[q, 3 + cl, 12:16, :] = south[it, q, cl]

        def first_guess(j, carry):
            for at in (0, 8):
                rows = pl.ds(at, 8)
                for q in range(2):
                    re, im = h[q, j, rows, :], h[q + 2, j, rows, :]
                    p_re, p_im, p_x = lead[0, q, j, rows, :], lead[1, q, j, rows, :], lead[2, q, j, rows, :]
                    wa[q, j, pl.ds(8 + at, 8), :] = p_re * re + p_x * im
                    wa[q + 2, j, pl.ds(8 + at, 8), :] = p_im * im - p_x * re
            return carry

        lax.fori_loop(0, 8, first_guess, 0)
        sweep(wa, wb, 1, 7)
        sweep(wb, wa, 2, 6)
        guess, image = [], []
        for cl in range(2):
            j = 3 + cl
            w_row, g_row = [None] * 4, [None] * 4
            for q in range(2):
                s_re, s_im, s_x = shifts(q)
                w_re, b_re = stencil(wa, q, j, 12, 8, 4)
                w_im, b_im = stencil(wa, q + 2, j, 12, 8, 4)
                w_row[q], w_row[q + 2] = w_re, w_im
                g_row[q] = b_re - (s_re * w_re + s_x * w_im)
                g_row[q + 2] = b_im - (s_im * w_im - s_x * w_re)
            mean = w_row[0] * small_ref[6:7, :]
            for q in range(1, 4):
                mean = mean + w_row[q] * small_ref[6 + q : 7 + q, :]
            corner = jnp.broadcast_to(jnp.sum(mean, axis=1, keepdims=True), (8, 128))
            g_row[0] = g_row[0] + corner
            g_row[1] = g_row[1] + corner
            g_row[2] = g_row[2] + jnp.where(lanes_below(1), corner, 0.0)
            guess.append(jnp.concatenate(w_row, axis=1))
            image.append(jnp.concatenate(g_row, axis=1))
        guess = jnp.concatenate(guess, axis=0)
        image = jnp.concatenate(image, axis=0)
        if it + 1 < KRYLOV:
            put_spectrum(it + 1, image)
            halo = send_halo(it + 1)
        both = jnp.dot(
            jnp.concatenate([guess, image], axis=0), inv[...], precision=HIGHEST, preferred_element_type=F32
        )
        directions.append(both[0:16])
        vectors.append(both[16:32])
        send_strip(it)
        for i in range(it + 2):
            grams[i, it + 1] = dot_pairs(vectors[i], vectors[it + 1])
        if it == 1:
            send_steps(0)

    order = [(i, j) for i in range(KRYLOV + 1) for j in range(i, KRYLOV + 1)]
    row_is = lax.broadcasted_iota(jnp.int32, (16, 128), 0)
    lane_is = lax.broadcasted_iota(jnp.int32, (16, 128), 1)
    high = jnp.zeros((16, 128), F32)
    low = jnp.zeros((16, 128), F32)
    for n, key in enumerate(order):
        a, b = grams[key]
        high = jnp.where(row_is == n, jnp.concatenate([a, a], axis=0), high)
        low = jnp.where(row_is == n, jnp.concatenate([b, b], axis=0), low)
    for shift in (64, 32, 16, 8, 4, 2, 1):
        high, t = two_sum(high, pltpu.roll(high, shift, 1))
        low = low + pltpu.roll(low, shift, 1) + t
    packed = jnp.where(lane_is == row_is, high, jnp.where(lane_is == row_is + 16, low, 0.0))
    mine = jnp.sum(packed, axis=0, keepdims=True)

    def add_start(mine, src, dst, s_sem, r_sem, devices, me):
        src[...] = mine
        dst[me] = mine
        return [send(src, dst.at[me], s_sem.at[d], r_sem.at[d], device) for d, device in devices]

    def add_end(copies, dst):
        for copy in copies:
            copy.wait_recv()
        level = [(dst[i], None) for i in range(len(copies) + 1)]
        while len(level) > 1:
            following = []
            for (a, ea), (b, eb) in zip(level[::2], level[1::2]):
                s, t = two_sum(a, b)
                for extra in (ea, eb):
                    t = t if extra is None else t + extra
                following.append((s, t))
            level = following
        s, t = level[0]
        lane = lax.broadcasted_iota(jnp.int32, (1, 128), 1)
        return s + jnp.where((lane >= 16) & (lane < 32), pltpu.roll(t, 16, 1), 0.0)

    adds = add_start(
        mine, ars1, ar1, a1_s, a1_r, [(d, place(((z + d) % 8) * 16 + e_me, x)) for d in FAR_8], z
    )
    send_steps(1)
    mine = add_end(adds, ar1)
    adds = add_start(mine, ars0, ar0, a0_s, a0_r, [(d, place(z * 16 + (e_me + d) % 16, x)) for d in FAR_16], e_me)
    send_steps(2)
    mine = add_end(adds, ar0)
    adds = add_start(mine, ars2, ar2, a2_s, a2_r, [(d, place(tm, (x + d) % 4)) for d in (2, 1, 3)], x)
    mine = add_end(adds, ar2)
    mine = jnp.broadcast_to(mine, (8, 128))
    gram = [[None] * (KRYLOV + 1) for _ in range(KRYLOV + 1)]
    for n, (i, j) in enumerate(order):
        value = (
            jnp.broadcast_to(mine[:, n : n + 1], (8, 128)),
            jnp.broadcast_to(mine[:, 16 + n : 17 + n], (8, 128)),
        )
        gram[i][j] = value
        gram[j][i] = value
    on_directions, on_vectors = krylov_weights(gram)

    for it in range(KRYLOV):
        for copy in stage4[it]:
            copy.wait_recv()
    sums = [[], []]
    for zz in range(8):
        total = on_directions[0] * r4[0, zz, 0]
        for it in range(1, KRYLOV):
            total = total + on_directions[it] * r4[it, zz, 0]
        sums[0].append(total)
        total = on_vectors[0] * m1[zz]
        for it in range(KRYLOV):
            total = total + on_vectors[it + 1] * r4[it, zz, 1]
        sums[1].append(total)
    for f, out in ((0, sol_ref), (1, res_ref)):
        for t in range(4):
            for hh in range(2):
                value = None
                for k in range(4):
                    piece = turn(sums[f][hh * 4 + k], k * 32 - t * 32)
                    value = piece if value is None else jnp.where(lane_block(k), piece, value)
                out[t, :, hh * 128 : hh * 128 + 128] = value
    for copy in started:
        copy.wait_send()


def per_device(right_side, diffusion, velocity):
    forward, inverse, small = tables()
    vmem = pl.BlockSpec(memory_space=pltpu.VMEM)
    hbm = pl.BlockSpec(memory_space=pltpu.HBM)

    def buffer(*shape):
        return pltpu.VMEM(shape, F32)

    def sems(*shape):
        return pltpu.SemaphoreType.DMA(shape)

    out = jax.ShapeDtypeStruct(right_side.shape, F32)
    return pl.pallas_call(
        kernel,
        out_shape=(out, out),
        in_specs=[hbm] * 6,
        out_specs=(vmem, vmem),
        scratch_shapes=[
            buffer(4, 8, 256), buffer(8, 256), buffer(2, 8, 256), buffer(16, 128), buffer(L, L), buffer(L, L),
            buffer(8, 8, 128), buffer(8, 8, 128), buffer(128, 128), buffer(16, 4, 128), buffer(16, 4, 128),
            buffer(3, 8, 256), buffer(3, 2, 8, 256),
            buffer(5, 8, 16, 128), buffer(3, 2, 8, 16, 128),
            buffer(3, 4, 2, 8, 128), buffer(3, 2, 4, 2, 4, 128), buffer(3, 2, 4, 2, 2, 128),
            buffer(4, 8, 16, 128),
            buffer(3, 4, 2, 8, 128), buffer(3, 4, 2, 8, 128), buffer(3, 4, 8, 128), buffer(3, 4, 8, 128),
            buffer(3, 4, 2, 4, 128), buffer(3, 4, 2, 4, 128),
            buffer(3, 4, 2, 2, 128), buffer(3, 4, 2, 2, 128), buffer(3, 4, 2, 2, 128), buffer(3, 4, 2, 2, 128),
            buffer(4, 8, 32, 128), buffer(4, 8, 32, 128),
            buffer(16, 1, 128), buffer(8, 1, 128), buffer(4, 1, 128),
            buffer(1, 128), buffer(1, 128), buffer(1, 128),
            buffer(3, 16, 8, 128), buffer(3, 16, 8, 128), buffer(128, 128),
            buffer(3, 8, 2, 8, 128), buffer(3, 8, 2, 8, 128),
            sems(6), sems(4), sems(4), sems(8), sems(8), sems(16), sems(16), sems(3, 10), sems(3, 10),
            sems(16), sems(16), sems(8), sems(8), sems(4), sems(4),
            sems(3, 16), sems(3, 16), sems(3, 8), sems(3, 8),
        ],
        compiler_params=pltpu.CompilerParams(
            collective_id=0, has_side_effects=True, vmem_limit_bytes=67_000_000
        ),
    )(right_side, diffusion, velocity, small, forward, inverse)


def solution(mesh):
    return jax.shard_map(
        per_device,
        mesh=mesh,
        in_specs=(P("tm", "space", None), P("space", None), P(None, "space", None)),
        out_specs=(P("tm", "space", None), P("tm", "space", None)),
        check_vma=False,
    )
```

```python
import math

import jax
import jax.numpy as jnp
import numpy as np
from jax import lax
from jax.experimental import pallas as pl
from jax.experimental.pallas import tpu as pltpu
from jax.sharding import PartitionSpec as P

L = 512
KRYLOV = 3
ALPHA = 0.05
DAMPING = 0.8
EPSILON = 1e-06
LOG_DECAY = math.log(ALPHA) / L
DECAY = math.exp(LOG_DECAY)
MESH = pl.DeviceIdType.MESH
HIGHEST = lax.Precision.HIGHEST
FAR_8 = (4, 3, 5, 2, 6, 1, 7)
FAR_32 = tuple((d, c) for c in (2, 1, 3, 0) for d in FAR_8 + (0,) if (d, c) != (0, 0))
FAR_16 = (8, 7, 9, 6, 10, 5, 11, 4, 12, 3, 13, 2, 14, 1, 15)
F32 = jnp.float32


def tables():
    n = np.arange(L)
    k = np.arange(L // 2)
    angle = 2.0 * np.pi * ((n[:, None] * k[None, :]) % L) / L
    real = np.cos(angle)
    imag = -np.sin(angle)
    imag[:, 0] = np.where(n % 2 == 0, 1.0, -1.0)
    packed = np.concatenate([real, imag], axis=1)
    scale = np.full(L, 2.0 / L)
    scale[0] = scale[L // 2] = 1.0 / L
    decays = DECAY ** n
    forward = packed * decays[:, None]
    inverse = (packed * scale[None, :]).T / decays[None, :]
    shift_real = DECAY * np.cos(2.0 * np.pi * k / L)
    shift_imag = DECAY * np.sin(2.0 * np.pi * k / L)
    shift_other = shift_real.copy()
    shift_other[0] = -DECAY
    shift_imag[0] = 0.0
    corner = np.concatenate([shift_real * scale[: L // 2], shift_imag * scale[L // 2 :]])
    corner[L // 2] = -DECAY / L
    rows = np.concatenate([shift_real, shift_other, shift_imag, corner]).reshape(10, 128)
    small = np.zeros((16, 128))
    small[:10] = rows
    return forward.astype(np.float32), inverse.astype(np.float32), small.astype(np.float32)


def two_sum(a, b):
    s = a + b
    t = s - a
    return s, (a - (s - t)) + (b - t)


def split(a):
    c = 4097.0 * a
    high = c - (c - a)
    return high, a - high


def two_prod(a, b):
    p = a * b
    ah, al = split(a)
    bh, bl = split(b)
    return p, ((ah * bh - p) + ah * bl + al * bh) + al * bl


def pair_div(a, b):
    safe = jnp.where(b[0] > 0.0, b[0], 1.0)
    q = jnp.where(b[0] > 0.0, a[0] / safe, 0.0)
    p, e = two_prod(q, b[0])
    rest = ((a[0] - p) - e) + (a[1] - q * b[1])
    r = jnp.where(b[0] > 0.0, rest / safe, 0.0)
    s = q + r
    return s, r - (s - q)


def pair_less(a, m, b):
    p, e = two_prod(m[0], b[0])
    e = e + (m[0] * b[1] + m[1] * b[0])
    s, t = two_sum(a[0], -p)
    t = t + (a[1] - e)
    h = s + t
    return h, t - (h - s)


def krylov_weights(gram):
    n = KRYLOV + 1
    lower = [[None] * n for _ in range(n)]
    norm = [None] * n
    cross = [[None] * n for _ in range(n)]
    for k in range(n):
        for i in range(k, n):
            value = gram[k][i]
            for m in range(k):
                value = pair_less(value, lower[i][m], cross[k][m])
            cross[i][k] = value
        head = cross[k][k]
        keep = head[0] > 0.0
        head = (jnp.where(keep, head[0], 0.0), jnp.where(keep, head[1], 0.0))
        norm[k] = head[0]
        for i in range(k + 1, n):
            lower[i][k] = pair_div(cross[i][k], head)
    low = [[None if v is None else v[0] for v in row] for row in lower]
    zero = jnp.zeros_like(norm[0])
    images = []
    for k in range(KRYLOV):
        image = [low[k + 1][i] for i in range(k + 1)] + [zero + 1.0]
        for m in range(k):
            for i in range(m + 2):
                image[i] = image[i] - low[k][m] * images[m][i]
        images.append(image)
    beta = jnp.sqrt(norm[0] + EPSILON)
    basis = [[1.0 / beta]]
    hessen = [[zero] * KRYLOV for _ in range(n)]
    for j in range(KRYLOV):
        work = [zero] * (j + 2)
        for k in range(j + 1):
            for i in range(k + 2):
                work[i] = work[i] + basis[j][k] * images[k][i]
        for i in range(j + 1):
            total = zero
            for k in range(i + 1):
                total = total + basis[i][k] * norm[k] * work[k]
            hessen[i][j] = total
        for i in range(j + 1):
            for k in range(i + 1):
                work[k] = work[k] - hessen[i][j] * basis[i][k]
        total = zero
        for k in range(j + 2):
            total = total + work[k] * work[k] * norm[k]
        length = jnp.sqrt(total + EPSILON)
        hessen[j + 1][j] = length
        basis.append([v / length for v in work])
    ortho = []
    upper = [[None] * KRYLOV for _ in range(KRYLOV)]
    for column in range(KRYLOV):
        current = [hessen[i][column] for i in range(n)]
        for row in range(column):
            factor = sum(ortho[row][i] * current[i] for i in range(n))
            upper[row][column] = factor
            current = [current[i] - factor * ortho[row][i] for i in range(n)]
        length = jnp.sqrt(sum(v * v for v in current))
        upper[column][column] = length
        ortho.append([v / length for v in current])
    values = [None] * KRYLOV
    for row in reversed(range(KRYLOV)):
        accum = ortho[row][0] * beta
        for later in range(row + 1, KRYLOV):
            accum = accum - upper[row][later] * values[later]
        values[row] = accum / upper[row][row]
    target = []
    for i in range(n):
        accum = beta if i == 0 else zero
        for j in range(KRYLOV):
            accum = accum - hessen[i][j] * values[j]
        target.append(accum)

    def on_p(weights):
        on_u = [zero] * len(weights)
        for j, weight in enumerate(weights):
            for k in range(len(basis[j])):
                if k < len(weights):
                    on_u[k] = on_u[k] + weight * basis[j][k]
        for k in reversed(range(len(weights))):
            for i in range(k):
                on_u[i] = on_u[i] - low[k][i] * on_u[k]
        return on_u

    return on_p(values), on_p(target)


def lanes_below(count, shape=(8, 128)):
    return lax.broadcasted_iota(jnp.int32, shape, len(shape) - 1) < count


def lane_block(index):
    lane = lax.broadcasted_iota(jnp.int32, (8, 128), 1)
    return (lane >= 32 * index) & (lane < 32 * index + 32)


def turn(value, amount):
    amount = amount % 128
    return value if amount == 0 else pltpu.roll(value, amount, 1)


def kernel(
    b_hbm, diff_hbm, vel_hbm, small_hbm, fwd_hbm, inv_hbm,
    sol_ref, res_ref,
    b_ref, diff_ref, vel_ref, small_ref, fwd, inv,
    m1, r1, buf1, m2, r2, cd, cv, point, lead, own, edge4, edge2, h,
    left1, right1, left2, right2, north, south, nw, ne, sw, se, wa, wb,
    ar0, ar1, ars0, ars1, m3, r3, buf2, m4, r4,
    const_sem, coef_s, coef_r, s1_s, s1_r, s2_s, s2_r, ha_s, ha_r, a0_s, a0_r, a1_s, a1_r,
    s3_s, s3_r, s4_s, s4_r,
):
    tm = lax.axis_index("tm")
    x = lax.axis_index("space")
    z = tm // 16
    e_me = tm % 16
    y = e_me // 2
    core = e_me % 2
    odd = z % 2
    ys = y + odd * (7 - 2 * y)
    g = (z * 8 + ys) * 2 + core

    def at_strip(index):
        index = (index + 128) % 128
        strip = index // 2
        zz = strip // 8
        yy = strip % 8
        yy = yy + (zz % 2) * (7 - 2 * yy)
        return zz * 16 + yy * 2 + index % 2

    def place(t, s):
        return {"tm": t, "space": s}

    up = (x + 3) % 4
    down = (x + 1) % 4
    loads = [
        pltpu.make_async_copy(src, dst, const_sem.at[i])
        for i, (src, dst) in enumerate(
            (
                (b_hbm, b_ref), (diff_hbm, diff_ref), (vel_hbm, vel_ref),
                (small_hbm, small_ref), (fwd_hbm, fwd), (inv_hbm, inv),
            )
        )
    ]
    loads[0].start()
    barrier = pltpu.get_barrier_semaphore()
    greet = [place(((z + d) % 8) * 16 + e_me, x) for d in FAR_8]
    greet += [place(z * 16 + (e_me + d) % 16, x) for d in FAR_16]
    greet += [place(tm, (x + d) % 4) for d in range(1, 4)]
    for d in (-2, -1, 1, 2):
        greet.append(place(at_strip(g + d), x))
    for d in (-1, 1):
        for s in (up, down):
            greet.append(place(at_strip(g + d), s))
    for device in greet:
        pl.semaphore_signal(barrier, inc=1, device_id=device, device_id_type=MESH)
    for copy in loads[1:]:
        copy.start()
    loads[0].wait()

    for zz in range(8):
        value = None
        for t in range(4):
            piece = turn(b_ref[t, :, (zz // 4) * 128 : (zz // 4) * 128 + 128], t * 32 - (zz % 4) * 32)
            value = piece if value is None else jnp.where(lane_block(t), piece, value)
        m1[zz] = value
    r1[z] = m1[z]
    loads[1].wait()
    loads[2].wait()

    pl.semaphore_wait(barrier, len(greet))

    started = []

    def send(src, dst, s_sem, r_sem, device):
        copy = pltpu.make_async_remote_copy(
            src_ref=src, dst_ref=dst, send_sem=s_sem, recv_sem=r_sem, device_id=device, device_id_type=MESH
        )
        copy.start()
        started.append(copy)
        return copy

    stage1 = [
        send(m1.at[(z + d) % 8], r1.at[z], s1_s.at[d], s1_r.at[d], place(((z + d) % 8) * 16 + e_me, x))
        for d in FAR_8
    ]
    coefs = [
        send(diff_ref, cd.at[2], coef_s.at[0], coef_r.at[0], place(tm, up)),
        send(vel_ref, cv.at[2], coef_s.at[1], coef_r.at[1], place(tm, up)),
        send(diff_ref, cd.at[0], coef_s.at[2], coef_r.at[2], place(tm, down)),
        send(vel_ref, cv.at[0], coef_s.at[3], coef_r.at[3], place(tm, down)),
    ]
    h[...] = jnp.zeros_like(h)
    wa[...] = jnp.zeros_like(wa)
    wb[...] = jnp.zeros_like(wb)
    cd[1] = diff_ref[...]
    cv[1] = vel_ref[...]
    loads[3].wait()
    for copy in stage1:
        copy.wait_recv()
    half = lanes_below(64, (16, 128))
    turned = jnp.transpose(r1[...].reshape(64, 128))
    buf1[:, 0:64] = turned
    for t in range(4):
        even = buf1[pl.ds(t * 32, 16, stride=2), :]
        other = buf1[pl.ds(t * 32 + 1, 16, stride=2), :]
        m2[:, t, :] = jnp.where(half, even, pltpu.roll(other, 64, 1))

    def strip_of(e):
        yy = e // 2
        return (yy + odd * (7 - 2 * yy)) * 2 + e % 2

    r2[e_me] = m2[strip_of(e_me)]
    stage2 = []
    for d in FAR_16:
        to = (e_me + d) % 16
        stage2.append(
            send(m2.at[strip_of(to)], r2.at[e_me], s2_s.at[d], s2_r.at[d], place(z * 16 + to, x))
        )

    for copy in coefs:
        copy.wait_recv()
    parts = []
    for prev, mine, after in (
        (cd[0], cd[1], cd[2]),
        (cv[0, 0], cv[1, 0], cv[2, 0]),
        (cv[0, 1], cv[1, 1], cv[2, 1]),
    ):
        parts += [prev[4:8], mine, after[0:4]]
    stacked = jnp.concatenate(parts, axis=0)
    row_at = lax.broadcasted_iota(jnp.int32, (256, 128), 0)
    for j in range(8):
        pick = jnp.where(row_at == 2 * g - 3 + j, 1.0, 0.0).astype(F32)
        spread = jnp.dot(stacked, pick, precision=HIGHEST, preferred_element_type=F32)
        diff = spread[0:16]
        v_col = spread[16:32]
        v_row = spread[32:48]
        diag = 1.0 + 4.0 * diff
        point[0, j] = diag
        point[1, j] = -diff - v_row
        point[2, j] = -diff + v_row
        point[3, j] = -diff - v_col
        point[4, j] = -diff + v_col
        row = 8 * x - 4 + lax.broadcasted_iota(jnp.int32, (16, 128), 0)
        column = 2 * g - 3 + j
        inside = (row >= 0) & (row < 32) & (column >= 0) & (column < 256)
        for q in range(2):
            d_i = small_ref[4 + q : 5 + q, :]
            for which, base in ((0, 0), (1, 2)):
                d_r = diag - small_ref[base + q : base + q + 1, :]
                scale = jnp.where(inside, DAMPING / (d_r * d_r + d_i * d_i), 0.0)
                lead[which, q, j] = d_r * scale
                if which == 0:
                    lead[2, q, j] = d_i * scale

    for copy in stage2:
        copy.wait_recv()
    turned = jnp.transpose(r2[...].reshape(64, 128))
    low64 = lanes_below(64)
    tiles = []
    for cl in range(2):
        row = []
        for a in range(4):
            v0 = turned[cl * 64 + a * 16 : cl * 64 + a * 16 + 8, :]
            v1 = turned[cl * 64 + a * 16 + 8 : cl * 64 + a * 16 + 16, :]
            row.append(jnp.concatenate([v0, v1], axis=1))
        tiles.append(jnp.concatenate(row, axis=1))
    field = jnp.concatenate(tiles, axis=0)
    loads[4].wait()
    loads[5].wait()
    spectrum = jnp.dot(field, fwd[...], precision=HIGHEST, preferred_element_type=F32)
    vectors = [field]
    directions = []

    def dot_pairs(a, b):
        high = low = None
        for cl in range(2):
            for q in range(4):
                va = a[cl * 8 : cl * 8 + 8, q * 128 : q * 128 + 128]
                vb = b[cl * 8 : cl * 8 + 8, q * 128 : q * 128 + 128]
                p, e = two_prod(va, vb)
                if high is None:
                    high, low = p, e
                else:
                    high, t = two_sum(high, p)
                    low = low + (t + e)
        for shift in (4, 2, 1):
            high, t = two_sum(high, pltpu.roll(high, shift, 0))
            low = low + pltpu.roll(low, shift, 0) + t
        return high, low

    grams = {}

    def put_spectrum(it, value):
        for q in range(4):
            for cl in range(2):
                own[it, q, cl] = value[cl * 8 : cl * 8 + 8, q * 128 : q * 128 + 128]
                edge4[it, 0, q, cl] = value[cl * 8 : cl * 8 + 4, q * 128 : q * 128 + 128]
                edge4[it, 1, q, cl] = value[cl * 8 + 4 : cl * 8 + 8, q * 128 : q * 128 + 128]
                edge2[it, 0, q, cl] = value[cl * 8 : cl * 8 + 2, q * 128 : q * 128 + 128]
                edge2[it, 1, q, cl] = value[cl * 8 + 6 : cl * 8 + 8, q * 128 : q * 128 + 128]

    def send_halo(it):
        n1, n2, p1, p2 = (at_strip(g - 1), at_strip(g - 2), at_strip(g + 1), at_strip(g + 2))
        moves = (
            (edge2.at[it, 1], nw.at[it], place(p1, down)),
            (edge2.at[it, 1], ne.at[it], place(n1, down)),
            (edge2.at[it, 0], sw.at[it], place(p1, up)),
            (edge2.at[it, 0], se.at[it], place(n1, up)),
            (own.at[it], left1.at[it], place(p1, x)),
            (own.at[it], right1.at[it], place(n1, x)),
            (edge4.at[it, 1], north.at[it], place(tm, down)),
            (edge4.at[it, 0], south.at[it], place(tm, up)),
            (own.at[it, :, 1], left2.at[it], place(p2, x)),
            (own.at[it, :, 0], right2.at[it], place(n2, x)),
        )
        return [
            send(src, dst, ha_s.at[it, i], ha_r.at[it, i], device)
            for i, (src, dst, device) in enumerate(moves)
        ]

    def shifts(q):
        return (small_ref[q : q + 1, :], small_ref[2 + q : 3 + q, :], small_ref[4 + q : 5 + q, :])

    def stencil(w, q, j, start, rows, at):
        here = w[q, j, pl.ds(start, rows), :]
        return here, (
            point[0, j, pl.ds(at, rows), :] * here
            + point[1, j, pl.ds(at, rows), :] * w[q, j, pl.ds(start - 1, rows), :]
            + point[2, j, pl.ds(at, rows), :] * w[q, j, pl.ds(start + 1, rows), :]
            + point[3, j, pl.ds(at, rows), :] * w[q, j - 1, pl.ds(start, rows), :]
            + point[4, j, pl.ds(at, rows), :] * w[q, j + 1, pl.ds(start, rows), :]
        )

    def sweep(source, target, first, last):
        def body(j, carry):
            for at in (0, 8):
                for q in range(2):
                    s_re, s_im, s_x = shifts(q)
                    w_re, b_re = stencil(source, q, j, 8 + at, 8, at)
                    w_im, b_im = stencil(source, q + 2, j, 8 + at, 8, at)
                    rows = pl.ds(at, 8)
                    left_re = h[q, j, rows, :] - (b_re - (s_re * w_re + s_x * w_im))
                    left_im = h[q + 2, j, rows, :] - (b_im - (s_im * w_im - s_x * w_re))
                    p_re, p_im, p_x = lead[0, q, j, rows, :], lead[1, q, j, rows, :], lead[2, q, j, rows, :]
                    target[q, j, pl.ds(8 + at, 8), :] = w_re + (p_re * left_re + p_x * left_im)
                    target[q + 2, j, pl.ds(8 + at, 8), :] = w_im + (p_im * left_im - p_x * left_re)
            return carry

        lax.fori_loop(first, last, body, 0)

    strip_me = strip_of(e_me)
    stage3, stage4 = {}, {}

    def pieces(value):
        return [[value[cl * 8 : cl * 8 + 8, q * 128 : q * 128 + 128] for q in range(4)] for cl in range(2)]

    def send_strip(it):
        p0, p1 = pieces(directions[it]), pieces(vectors[it + 1])
        rows = []
        for cl in range(2):
            for a in range(4):
                f0, f1 = p0[cl][a], p1[cl][a]
                rows.append(jnp.where(low64, f0, pltpu.roll(f1, 64, 1)))
                rows.append(jnp.where(low64, pltpu.roll(f0, 64, 1), f1))
        turned = jnp.transpose(jnp.concatenate(rows, axis=0))
        for src in range(16):
            for f in range(2):
                m3[it, src, f * 4 : f * 4 + 4, :] = turned[f * 64 + src * 4 : f * 64 + src * 4 + 4, :]
        r3[it, strip_me] = m3[it, e_me]
        stage3[it] = []
        for d in FAR_16:
            to = (e_me + d) % 16
            stage3[it].append(
                send(m3.at[it, to], r3.at[it, strip_me], s3_s.at[it, d], s3_r.at[it, d], place(z * 16 + to, x))
            )

    def send_steps(it):
        for copy in stage3[it]:
            copy.wait_recv()
        for t in range(4):
            f0 = r3[it, :, t, :]
            f1 = r3[it, :, 4 + t, :]
            buf2[pl.ds(t * 32, 16, stride=2), :] = jnp.where(half, f0, pltpu.roll(f1, 64, 1))
            buf2[pl.ds(t * 32 + 1, 16, stride=2), :] = jnp.where(half, pltpu.roll(f0, 64, 1), f1)
        turned = jnp.transpose(buf2[...])
        for zz in range(8):
            for f in range(2):
                m4[it, zz, f] = turned[f * 64 + zz * 8 : f * 64 + zz * 8 + 8, :]
        r4[it, z] = m4[it, z]
        stage4[it] = [
            send(
                m4.at[it, (z + d) % 8], r4.at[it, z], s4_s.at[it, d], s4_r.at[it, d],
                place(((z + d) % 8) * 16 + e_me, x),
            )
            for d in FAR_8
        ]

    put_spectrum(0, spectrum)
    halo = send_halo(0)
    grams[0, 0] = dot_pairs(field, field)

    for it in range(KRYLOV):
        for q in range(4):
            for cl in range(2):
                h[q, 3 + cl, 4:12, :] = own[it, q, cl]
        for copy in halo:
            copy.wait_recv()
        for q in range(4):
            h[q, 0, 4:12, :] = left2[it, q]
            h[q, 7, 4:12, :] = right2[it, q]
            for cl in range(2):
                h[q, 1 + cl, 4:12, :] = left1[it, q, cl]
                h[q, 1 + cl, 2:4, :] = nw[it, q, cl]
                h[q, 1 + cl, 12:14, :] = sw[it, q, cl]
                h[q, 5 + cl, 4:12, :] = right1[it, q, cl]
                h[q, 5 + cl, 2:4, :] = ne[it, q, cl]
                h[q, 5 + cl, 12:14, :] = se[it, q, cl]
                h[q, 3 + cl, 0:4, :] = north[it, q, cl]
                h[q, 3 + cl, 12:16, :] = south[it, q, cl]

        def first_guess(j, carry):
            for at in (0, 8):
                rows = pl.ds(at, 8)
                for q in range(2):
                    re, im = h[q, j, rows, :], h[q + 2, j, rows, :]
                    p_re, p_im, p_x = lead[0, q, j, rows, :], lead[1, q, j, rows, :], lead[2, q, j, rows, :]
                    wa[q, j, pl.ds(8 + at, 8), :] = p_re * re + p_x * im
                    wa[q + 2, j, pl.ds(8 + at, 8), :] = p_im * im - p_x * re
            return carry

        lax.fori_loop(0, 8, first_guess, 0)
        sweep(wa, wb, 1, 7)
        sweep(wb, wa, 2, 6)
        guess, image = [], []
        for cl in range(2):
            j = 3 + cl
            w_row, g_row = [None] * 4, [None] * 4
            for q in range(2):
                s_re, s_im, s_x = shifts(q)
                w_re, b_re = stencil(wa, q, j, 12, 8, 4)
                w_im, b_im = stencil(wa, q + 2, j, 12, 8, 4)
                w_row[q], w_row[q + 2] = w_re, w_im
                g_row[q] = b_re - (s_re * w_re + s_x * w_im)
                g_row[q + 2] = b_im - (s_im * w_im - s_x * w_re)
            mean = w_row[0] * small_ref[6:7, :]
            for q in range(1, 4):
                mean = mean + w_row[q] * small_ref[6 + q : 7 + q, :]
            corner = jnp.broadcast_to(jnp.sum(mean, axis=1, keepdims=True), (8, 128))
            g_row[0] = g_row[0] + corner
            g_row[1] = g_row[1] + corner
            g_row[2] = g_row[2] + jnp.where(lanes_below(1), corner, 0.0)
            guess.append(jnp.concatenate(w_row, axis=1))
            image.append(jnp.concatenate(g_row, axis=1))
        guess = jnp.concatenate(guess, axis=0)
        image = jnp.concatenate(image, axis=0)
        if it + 1 < KRYLOV:
            put_spectrum(it + 1, image)
            halo = send_halo(it + 1)
        both = jnp.dot(
            jnp.concatenate([guess, image], axis=0), inv[...], precision=HIGHEST, preferred_element_type=F32
        )
        directions.append(both[0:16])
        vectors.append(both[16:32])
        send_strip(it)
        for i in range(it + 2):
            grams[i, it + 1] = dot_pairs(vectors[i], vectors[it + 1])
        if it == 1:
            send_steps(0)

    order = [(i, j) for i in range(KRYLOV + 1) for j in range(i, KRYLOV + 1)]
    row_is = lax.broadcasted_iota(jnp.int32, (16, 128), 0)
    lane_is = lax.broadcasted_iota(jnp.int32, (16, 128), 1)
    high = jnp.zeros((16, 128), F32)
    low = jnp.zeros((16, 128), F32)
    for n, key in enumerate(order):
        a, b = grams[key]
        high = jnp.where(row_is == n, jnp.concatenate([a, a], axis=0), high)
        low = jnp.where(row_is == n, jnp.concatenate([b, b], axis=0), low)
    for shift in (64, 32, 16, 8, 4, 2, 1):
        high, t = two_sum(high, pltpu.roll(high, shift, 1))
        low = low + pltpu.roll(low, shift, 1) + t
    packed = jnp.where(lane_is == row_is, high, jnp.where(lane_is == row_is + 16, low, 0.0))
    mine = jnp.sum(packed, axis=0, keepdims=True)

    def add_start(mine, src, dst, s_sem, r_sem, devices, me):
        src[...] = mine
        dst[me] = mine
        return [send(src, dst.at[me], s_sem.at[d], r_sem.at[d], device) for d, device in devices]

    def add_end(copies, dst):
        for copy in copies:
            copy.wait_recv()
        level = [(dst[i], None) for i in range(len(copies) + 1)]
        while len(level) > 1:
            following = []
            for (a, ea), (b, eb) in zip(level[::2], level[1::2]):
                s, t = two_sum(a, b)
                for extra in (ea, eb):
                    t = t if extra is None else t + extra
                following.append((s, t))
            level = following
        s, t = level[0]
        lane = lax.broadcasted_iota(jnp.int32, (1, 128), 1)
        return s + jnp.where((lane >= 16) & (lane < 32), pltpu.roll(t, 16, 1), 0.0)

    others = [
        (d * 4 + c, place(((z + d) % 8) * 16 + e_me, (x + c) % 4)) for d, c in FAR_32
    ]
    adds = add_start(mine, ars1, ar1, a1_s, a1_r, others, z * 4 + x)
    send_steps(1)
    mine = add_end(adds, ar1)
    adds = add_start(mine, ars0, ar0, a0_s, a0_r, [(d, place(z * 16 + (e_me + d) % 16, x)) for d in FAR_16], e_me)
    send_steps(2)
    mine = add_end(adds, ar0)
    mine = jnp.broadcast_to(mine, (8, 128))
    gram = [[None] * (KRYLOV + 1) for _ in range(KRYLOV + 1)]
    for n, (i, j) in enumerate(order):
        value = (
            jnp.broadcast_to(mine[:, n : n + 1], (8, 128)),
            jnp.broadcast_to(mine[:, 16 + n : 17 + n], (8, 128)),
        )
        gram[i][j] = value
        gram[j][i] = value
    on_directions, on_vectors = krylov_weights(gram)

    for it in range(KRYLOV):
        for copy in stage4[it]:
            copy.wait_recv()
    sums = [[], []]
    for zz in range(8):
        total = on_directions[0] * r4[0, zz, 0]
        for it in range(1, KRYLOV):
            total = total + on_directions[it] * r4[it, zz, 0]
        sums[0].append(total)
        total = on_vectors[0] * m1[zz]
        for it in range(KRYLOV):
            total = total + on_vectors[it + 1] * r4[it, zz, 1]
        sums[1].append(total)
    for f, out in ((0, sol_ref), (1, res_ref)):
        for t in range(4):
            for hh in range(2):
                value = None
                for k in range(4):
                    piece = turn(sums[f][hh * 4 + k], k * 32 - t * 32)
                    value = piece if value is None else jnp.where(lane_block(k), piece, value)
                out[t, :, hh * 128 : hh * 128 + 128] = value
    for copy in started:
        copy.wait_send()


def per_device(right_side, diffusion, velocity):
    forward, inverse, small = tables()
    vmem = pl.BlockSpec(memory_space=pltpu.VMEM)
    hbm = pl.BlockSpec(memory_space=pltpu.HBM)

    def buffer(*shape):
        return pltpu.VMEM(shape, F32)

    def sems(*shape):
        return pltpu.SemaphoreType.DMA(shape)

    out = jax.ShapeDtypeStruct(right_side.shape, F32)
    return pl.pallas_call(
        kernel,
        out_shape=(out, out),
        in_specs=[hbm] * 6,
        out_specs=(vmem, vmem),
        scratch_shapes=[
            buffer(4, 8, 256), buffer(8, 256), buffer(2, 8, 256), buffer(16, 128), buffer(L, L), buffer(L, L),
            buffer(8, 8, 128), buffer(8, 8, 128), buffer(128, 128), buffer(16, 4, 128), buffer(16, 4, 128),
            buffer(3, 8, 256), buffer(3, 2, 8, 256),
            buffer(5, 8, 16, 128), buffer(3, 2, 8, 16, 128),
            buffer(3, 4, 2, 8, 128), buffer(3, 2, 4, 2, 4, 128), buffer(3, 2, 4, 2, 2, 128),
            buffer(4, 8, 16, 128),
            buffer(3, 4, 2, 8, 128), buffer(3, 4, 2, 8, 128), buffer(3, 4, 8, 128), buffer(3, 4, 8, 128),
            buffer(3, 4, 2, 4, 128), buffer(3, 4, 2, 4, 128),
            buffer(3, 4, 2, 2, 128), buffer(3, 4, 2, 2, 128), buffer(3, 4, 2, 2, 128), buffer(3, 4, 2, 2, 128),
            buffer(4, 8, 32, 128), buffer(4, 8, 32, 128),
            buffer(16, 1, 128), buffer(32, 1, 128), buffer(1, 128), buffer(1, 128),
            buffer(3, 16, 8, 128), buffer(3, 16, 8, 128), buffer(128, 128),
            buffer(3, 8, 2, 8, 128), buffer(3, 8, 2, 8, 128),
            sems(6), sems(4), sems(4), sems(8), sems(8), sems(16), sems(16), sems(3, 10), sems(3, 10),
            sems(16), sems(16), sems(32), sems(32),
            sems(3, 16), sems(3, 16), sems(3, 8), sems(3, 8),
        ],
        compiler_params=pltpu.CompilerParams(
            collective_id=0, has_side_effects=True, vmem_limit_bytes=40_000_000
        ),
    )(*[pltpu.with_memory_space_constraint(v, pltpu.HBM) for v in (right_side, diffusion, velocity, jnp.asarray(small), jnp.asarray(forward), jnp.asarray(inverse))])


def solution(mesh):
    return jax.shard_map(
        per_device,
        mesh=mesh,
        in_specs=(P("tm", "space", None), P("space", None), P(None, "space", None)),
        out_specs=(P("tm", "space", None), P("tm", "space", None)),
        check_vma=False,
    )
```

```python
import math

import jax
import jax.numpy as jnp
import numpy as np
from jax import lax
from jax.experimental import pallas as pl
from jax.experimental.pallas import tpu as pltpu
from jax.sharding import PartitionSpec as P

L = 512
KRYLOV = 3
ALPHA = 0.05
DAMPING = 0.8
EPSILON = 1e-06
LOG_DECAY = math.log(ALPHA) / L
DECAY = math.exp(LOG_DECAY)
MESH = pl.DeviceIdType.MESH
HIGHEST = lax.Precision.HIGHEST
FAR_8 = (4, 3, 5, 2, 6, 1, 7)
FAR_32 = tuple((d, c) for c in (2, 1, 3, 0) for d in FAR_8 + (0,) if (d, c) != (0, 0))
FAR_16 = (8, 7, 9, 6, 10, 5, 11, 4, 12, 3, 13, 2, 14, 1, 15)
F32 = jnp.float32


def tables():
    n = np.arange(L)
    k = np.arange(L // 2)
    angle = 2.0 * np.pi * ((n[:, None] * k[None, :]) % L) / L
    real = np.cos(angle)
    imag = -np.sin(angle)
    imag[:, 0] = np.where(n % 2 == 0, 1.0, -1.0)
    packed = np.concatenate([real, imag], axis=1)
    scale = np.full(L, 2.0 / L)
    scale[0] = scale[L // 2] = 1.0 / L
    decays = DECAY ** n
    forward = packed * decays[:, None]
    inverse = (packed * scale[None, :]).T / decays[None, :]
    shift_real = DECAY * np.cos(2.0 * np.pi * k / L)
    shift_imag = DECAY * np.sin(2.0 * np.pi * k / L)
    shift_other = shift_real.copy()
    shift_other[0] = -DECAY
    shift_imag[0] = 0.0
    corner = np.concatenate([shift_real * scale[: L // 2], shift_imag * scale[L // 2 :]])
    corner[L // 2] = -DECAY / L
    rows = np.concatenate([shift_real, shift_other, shift_imag, corner]).reshape(10, 128)
    small = np.zeros((16, 128))
    small[:10] = rows
    return forward.astype(np.float32), inverse.astype(np.float32), small.astype(np.float32)


def two_sum(a, b):
    s = a + b
    t = s - a
    return s, (a - (s - t)) + (b - t)


def split(a):
    c = 4097.0 * a
    high = c - (c - a)
    return high, a - high


def two_prod(a, b):
    p = a * b
    ah, al = split(a)
    bh, bl = split(b)
    return p, ((ah * bh - p) + ah * bl + al * bh) + al * bl


def pair_div(a, b):
    safe = jnp.where(b[0] > 0.0, b[0], 1.0)
    q = jnp.where(b[0] > 0.0, a[0] / safe, 0.0)
    p, e = two_prod(q, b[0])
    rest = ((a[0] - p) - e) + (a[1] - q * b[1])
    r = jnp.where(b[0] > 0.0, rest / safe, 0.0)
    s = q + r
    return s, r - (s - q)


def pair_less(a, m, b):
    p, e = two_prod(m[0], b[0])
    e = e + (m[0] * b[1] + m[1] * b[0])
    s, t = two_sum(a[0], -p)
    t = t + (a[1] - e)
    h = s + t
    return h, t - (h - s)


def krylov_weights(gram):
    n = KRYLOV + 1
    lower = [[None] * n for _ in range(n)]
    norm = [None] * n
    cross = [[None] * n for _ in range(n)]
    for k in range(n):
        for i in range(k, n):
            value = gram[k][i]
            for m in range(k):
                value = pair_less(value, lower[i][m], cross[k][m])
            cross[i][k] = value
        head = cross[k][k]
        keep = head[0] > 0.0
        head = (jnp.where(keep, head[0], 0.0), jnp.where(keep, head[1], 0.0))
        norm[k] = head[0]
        for i in range(k + 1, n):
            lower[i][k] = pair_div(cross[i][k], head)
    low = [[None if v is None else v[0] for v in row] for row in lower]
    zero = jnp.zeros_like(norm[0])
    images = []
    for k in range(KRYLOV):
        image = [low[k + 1][i] for i in range(k + 1)] + [zero + 1.0]
        for m in range(k):
            for i in range(m + 2):
                image[i] = image[i] - low[k][m] * images[m][i]
        images.append(image)
    beta = jnp.sqrt(norm[0] + EPSILON)
    basis = [[1.0 / beta]]
    hessen = [[zero] * KRYLOV for _ in range(n)]
    for j in range(KRYLOV):
        work = [zero] * (j + 2)
        for k in range(j + 1):
            for i in range(k + 2):
                work[i] = work[i] + basis[j][k] * images[k][i]
        for i in range(j + 1):
            total = zero
            for k in range(i + 1):
                total = total + basis[i][k] * norm[k] * work[k]
            hessen[i][j] = total
        for i in range(j + 1):
            for k in range(i + 1):
                work[k] = work[k] - hessen[i][j] * basis[i][k]
        total = zero
        for k in range(j + 2):
            total = total + work[k] * work[k] * norm[k]
        length = jnp.sqrt(total + EPSILON)
        hessen[j + 1][j] = length
        basis.append([v / length for v in work])
    ortho = []
    upper = [[None] * KRYLOV for _ in range(KRYLOV)]
    for column in range(KRYLOV):
        current = [hessen[i][column] for i in range(n)]
        for row in range(column):
            factor = sum(ortho[row][i] * current[i] for i in range(n))
            upper[row][column] = factor
            current = [current[i] - factor * ortho[row][i] for i in range(n)]
        length = jnp.sqrt(sum(v * v for v in current))
        upper[column][column] = length
        ortho.append([v / length for v in current])
    values = [None] * KRYLOV
    for row in reversed(range(KRYLOV)):
        accum = ortho[row][0] * beta
        for later in range(row + 1, KRYLOV):
            accum = accum - upper[row][later] * values[later]
        values[row] = accum / upper[row][row]
    target = []
    for i in range(n):
        accum = beta if i == 0 else zero
        for j in range(KRYLOV):
            accum = accum - hessen[i][j] * values[j]
        target.append(accum)

    def on_p(weights):
        on_u = [zero] * len(weights)
        for j, weight in enumerate(weights):
            for k in range(len(basis[j])):
                if k < len(weights):
                    on_u[k] = on_u[k] + weight * basis[j][k]
        for k in reversed(range(len(weights))):
            for i in range(k):
                on_u[i] = on_u[i] - low[k][i] * on_u[k]
        return on_u

    return on_p(values), on_p(target)


def lanes_below(count, shape=(8, 128)):
    return lax.broadcasted_iota(jnp.int32, shape, len(shape) - 1) < count


def lane_block(index):
    lane = lax.broadcasted_iota(jnp.int32, (8, 128), 1)
    return (lane >= 32 * index) & (lane < 32 * index + 32)


def turn(value, amount):
    amount = amount % 128
    return value if amount == 0 else pltpu.roll(value, amount, 1)


def kernel(
    b_hbm, diff_hbm, vel_hbm, small_hbm, fwd_hbm, inv_hbm,
    out_ref,
    b_ref, diff_ref, vel_ref, small_ref, fwd, inv,
    m1, r1, buf1, m2, r2, cd, cv, point, lead, own, edge4, edge2, h,
    left1, right1, left2, right2, north, south, nw, ne, sw, se, wa, wb,
    ar0, ar1, ars0, ars1, m3, r3, buf2, m4, r4,
    const_sem, coef_s, coef_r, s1_s, s1_r, s2_s, s2_r, ha_s, ha_r, a0_s, a0_r, a1_s, a1_r,
    s3_s, s3_r, s4_s, s4_r,
):
    tm = lax.axis_index("tm")
    x = lax.axis_index("space")
    z = tm // 16
    e_me = tm % 16
    y = e_me // 2
    core = e_me % 2
    odd = z % 2
    ys = y + odd * (7 - 2 * y)
    g = (z * 8 + ys) * 2 + core

    def at_strip(index):
        index = (index + 128) % 128
        strip = index // 2
        zz = strip // 8
        yy = strip % 8
        yy = yy + (zz % 2) * (7 - 2 * yy)
        return zz * 16 + yy * 2 + index % 2

    def place(t, s):
        return {"tm": t, "space": s}

    up = (x + 3) % 4
    down = (x + 1) % 4
    loads = [
        pltpu.make_async_copy(src, dst, const_sem.at[i])
        for i, (src, dst) in enumerate(
            (
                (b_hbm, b_ref), (diff_hbm, diff_ref), (vel_hbm, vel_ref),
                (small_hbm, small_ref), (fwd_hbm, fwd), (inv_hbm, inv),
            )
        )
    ]
    loads[0].start()
    barrier = pltpu.get_barrier_semaphore()
    greet = [place(((z + d) % 8) * 16 + e_me, x) for d in FAR_8]
    greet += [place(z * 16 + (e_me + d) % 16, x) for d in FAR_16]
    greet += [place(tm, up), place(tm, down)]
    for d in (-1, 1):
        for s in (up, down):
            greet.append(place(at_strip(g + d), s))
    for device in greet:
        pl.semaphore_signal(barrier, inc=1, device_id=device, device_id_type=MESH)
    for copy in loads[1:]:
        copy.start()
    loads[0].wait()

    for zz in range(8):
        value = None
        for t in range(4):
            piece = turn(b_ref[t, :, (zz // 4) * 128 : (zz // 4) * 128 + 128], t * 32 - (zz % 4) * 32)
            value = piece if value is None else jnp.where(lane_block(t), piece, value)
        m1[zz] = value
    r1[z] = m1[z]
    loads[1].wait()
    loads[2].wait()

    pl.semaphore_wait(barrier, len(greet))

    started = []

    def send(src, dst, s_sem, r_sem, device):
        copy = pltpu.make_async_remote_copy(
            src_ref=src, dst_ref=dst, send_sem=s_sem, recv_sem=r_sem, device_id=device, device_id_type=MESH
        )
        copy.start()
        started.append(copy)
        return copy

    stage1 = [
        send(m1.at[(z + d) % 8], r1.at[z], s1_s.at[d], s1_r.at[d], place(((z + d) % 8) * 16 + e_me, x))
        for d in FAR_8
    ]
    coefs = [
        send(diff_ref, cd.at[2], coef_s.at[0], coef_r.at[0], place(tm, up)),
        send(vel_ref, cv.at[2], coef_s.at[1], coef_r.at[1], place(tm, up)),
        send(diff_ref, cd.at[0], coef_s.at[2], coef_r.at[2], place(tm, down)),
        send(vel_ref, cv.at[0], coef_s.at[3], coef_r.at[3], place(tm, down)),
    ]
    h[...] = jnp.zeros_like(h)
    wa[...] = jnp.zeros_like(wa)
    wb[...] = jnp.zeros_like(wb)
    cd[1] = diff_ref[...]
    cv[1] = vel_ref[...]
    loads[3].wait()
    for copy in stage1:
        copy.wait_recv()
    half = lanes_below(64, (16, 128))
    turned = jnp.transpose(r1[...].reshape(64, 128))
    buf1[:, 0:64] = turned
    for t in range(4):
        even = buf1[pl.ds(t * 32, 16, stride=2), :]
        other = buf1[pl.ds(t * 32 + 1, 16, stride=2), :]
        m2[:, t, :] = jnp.where(half, even, pltpu.roll(other, 64, 1))

    def strip_of(e):
        yy = e // 2
        return (yy + odd * (7 - 2 * yy)) * 2 + e % 2

    r2[e_me] = m2[strip_of(e_me)]
    stage2 = []
    for d in FAR_16:
        to = (e_me + d) % 16
        stage2.append(
            send(m2.at[strip_of(to)], r2.at[e_me], s2_s.at[d], s2_r.at[d], place(z * 16 + to, x))
        )

    for copy in coefs:
        copy.wait_recv()
    parts = []
    for prev, mine, after in (
        (cd[0], cd[1], cd[2]),
        (cv[0, 0], cv[1, 0], cv[2, 0]),
        (cv[0, 1], cv[1, 1], cv[2, 1]),
    ):
        parts += [prev[4:8], mine, after[0:4]]
    stacked = jnp.concatenate(parts, axis=0)
    row_at = lax.broadcasted_iota(jnp.int32, (256, 128), 0)
    for j in range(8):
        pick = jnp.where(row_at == 2 * g - 3 + j, 1.0, 0.0).astype(F32)
        spread = jnp.dot(stacked, pick, precision=HIGHEST, preferred_element_type=F32)
        diff = spread[0:16]
        v_col = spread[16:32]
        v_row = spread[32:48]
        diag = 1.0 + 4.0 * diff
        point[0, j] = diag
        point[1, j] = -diff - v_row
        point[2, j] = -diff + v_row
        point[3, j] = -diff - v_col
        point[4, j] = -diff + v_col
        row = 8 * x - 4 + lax.broadcasted_iota(jnp.int32, (16, 128), 0)
        column = 2 * g - 3 + j
        inside = (row >= 0) & (row < 32) & (column >= 0) & (column < 256)
        for q in range(2):
            d_i = small_ref[4 + q : 5 + q, :]
            for which, base in ((0, 0), (1, 2)):
                d_r = diag - small_ref[base + q : base + q + 1, :]
                scale = jnp.where(inside, DAMPING / (d_r * d_r + d_i * d_i), 0.0)
                lead[which, q, j] = d_r * scale
                if which == 0:
                    lead[2, q, j] = d_i * scale

    for copy in stage2:
        copy.wait_recv()
    turned = jnp.transpose(r2[...].reshape(64, 128))
    low64 = lanes_below(64)
    tiles = []
    for cl in range(2):
        row = []
        for a in range(4):
            v0 = turned[cl * 64 + a * 16 : cl * 64 + a * 16 + 8, :]
            v1 = turned[cl * 64 + a * 16 + 8 : cl * 64 + a * 16 + 16, :]
            row.append(jnp.concatenate([v0, v1], axis=1))
        tiles.append(jnp.concatenate(row, axis=1))
    field = jnp.concatenate(tiles, axis=0)
    loads[4].wait()
    loads[5].wait()
    spectrum = jnp.dot(field, fwd[...], precision=HIGHEST, preferred_element_type=F32)
    vectors = [field]
    directions = []

    def dot_pairs(a, b):
        high = low = None
        for cl in range(2):
            for q in range(4):
                va = a[cl * 8 : cl * 8 + 8, q * 128 : q * 128 + 128]
                vb = b[cl * 8 : cl * 8 + 8, q * 128 : q * 128 + 128]
                p, e = two_prod(va, vb)
                if high is None:
                    high, low = p, e
                else:
                    high, t = two_sum(high, p)
                    low = low + (t + e)
        for shift in (4, 2, 1):
            high, t = two_sum(high, pltpu.roll(high, shift, 0))
            low = low + pltpu.roll(low, shift, 0) + t
        return high, low

    grams = {}

    def put_spectrum(it, value):
        for q in range(4):
            for cl in range(2):
                own[it, q, cl] = value[cl * 8 : cl * 8 + 8, q * 128 : q * 128 + 128]
                edge4[it, 0, q, cl] = value[cl * 8 : cl * 8 + 4, q * 128 : q * 128 + 128]
                edge4[it, 1, q, cl] = value[cl * 8 + 4 : cl * 8 + 8, q * 128 : q * 128 + 128]
                edge2[it, 0, q, cl] = value[cl * 8 : cl * 8 + 2, q * 128 : q * 128 + 128]
                edge2[it, 1, q, cl] = value[cl * 8 + 6 : cl * 8 + 8, q * 128 : q * 128 + 128]

    def send_halo(it):
        n1, n2, p1, p2 = (at_strip(g - 1), at_strip(g - 2), at_strip(g + 1), at_strip(g + 2))
        moves = (
            (edge2.at[it, 1], nw.at[it], place(p1, down)),
            (edge2.at[it, 1], ne.at[it], place(n1, down)),
            (edge2.at[it, 0], sw.at[it], place(p1, up)),
            (edge2.at[it, 0], se.at[it], place(n1, up)),
            (own.at[it], left1.at[it], place(p1, x)),
            (own.at[it], right1.at[it], place(n1, x)),
            (edge4.at[it, 1], north.at[it], place(tm, down)),
            (edge4.at[it, 0], south.at[it], place(tm, up)),
            (own.at[it, :, 1], left2.at[it], place(p2, x)),
            (own.at[it, :, 0], right2.at[it], place(n2, x)),
        )
        return [
            send(src, dst, ha_s.at[it, i], ha_r.at[it, i], device)
            for i, (src, dst, device) in enumerate(moves)
        ]

    shifts = [
        [jnp.broadcast_to(small_ref[2 * k + q : 2 * k + q + 1, :], (8, 128)) for k in range(3)] for q in range(2)
    ]

    def weights_of(j, at):
        return [point[k, j, pl.ds(at, 8), :] for k in range(5)]

    def stencil(w, q, j, start, weights):
        here = w[q, j, pl.ds(start, 8), :]
        return here, (
            weights[0] * here
            + weights[1] * w[q, j, pl.ds(start - 1, 8), :]
            + weights[2] * w[q, j, pl.ds(start + 1, 8), :]
            + weights[3] * w[q, j - 1, pl.ds(start, 8), :]
            + weights[4] * w[q, j + 1, pl.ds(start, 8), :]
        )

    def sweep(source, target, first, last):
        def body(j, carry):
            done = []
            for at in (0, 8):
                weights = weights_of(j, at)
                for q in range(2):
                    s_re, s_im, s_x = shifts[q]
                    w_re, b_re = stencil(source, q, j, 8 + at, weights)
                    w_im, b_im = stencil(source, q + 2, j, 8 + at, weights)
                    rows = pl.ds(at, 8)
                    left_re = h[q, j, rows, :] - (b_re - (s_re * w_re + s_x * w_im))
                    left_im = h[q + 2, j, rows, :] - (b_im - (s_im * w_im - s_x * w_re))
                    p_re, p_im, p_x = lead[0, q, j, rows, :], lead[1, q, j, rows, :], lead[2, q, j, rows, :]
                    done.append((q, at, w_re + (p_re * left_re + p_x * left_im)))
                    done.append((q + 2, at, w_im + (p_im * left_im - p_x * left_re)))
            for q, at, value in done:
                target[q, j, pl.ds(8 + at, 8), :] = value
            return carry

        lax.fori_loop(first, last, body, 0, unroll=2)

    def guess_on(j, first, rows):
        at = pl.ds(first, rows)
        done = []
        for q in range(2):
            re, im = h[q, j, at, :], h[q + 2, j, at, :]
            p_re, p_im, p_x = lead[0, q, j, at, :], lead[1, q, j, at, :], lead[2, q, j, at, :]
            done.append((q, p_re * re + p_x * im))
            done.append((q + 2, p_im * im - p_x * re))
        for q, value in done:
            wa[q, j, pl.ds(8 + first, rows), :] = value

    strip_me = strip_of(e_me)
    stage3, stage4 = {}, {}

    def pieces(value):
        return [[value[cl * 8 : cl * 8 + 8, q * 128 : q * 128 + 128] for q in range(4)] for cl in range(2)]

    def send_strip(it):
        p0, p1 = pieces(directions[it]), pieces(vectors[it + 1])
        rows = []
        for cl in range(2):
            for a in range(4):
                f0, f1 = p0[cl][a], p1[cl][a]
                rows.append(jnp.where(low64, f0, pltpu.roll(f1, 64, 1)))
                rows.append(jnp.where(low64, pltpu.roll(f0, 64, 1), f1))
        turned = jnp.transpose(jnp.concatenate(rows, axis=0))
        for src in range(16):
            for f in range(2):
                m3[it, src, f * 4 : f * 4 + 4, :] = turned[f * 64 + src * 4 : f * 64 + src * 4 + 4, :]
        r3[it, strip_me] = m3[it, e_me]
        stage3[it] = []
        for d in FAR_16:
            to = (e_me + d) % 16
            stage3[it].append(
                send(m3.at[it, to], r3.at[it, strip_me], s3_s.at[it, d], s3_r.at[it, d], place(z * 16 + to, x))
            )

    def send_steps(it):
        for copy in stage3[it]:
            copy.wait_recv()
        for t in range(4):
            f0 = r3[it, :, t, :]
            f1 = r3[it, :, 4 + t, :]
            buf2[pl.ds(t * 32, 16, stride=2), :] = jnp.where(half, f0, pltpu.roll(f1, 64, 1))
            buf2[pl.ds(t * 32 + 1, 16, stride=2), :] = jnp.where(half, pltpu.roll(f0, 64, 1), f1)
        turned = jnp.transpose(buf2[...])
        for zz in range(8):
            for f in range(2):
                m4[it, zz, f] = turned[f * 64 + zz * 8 : f * 64 + zz * 8 + 8, :]
        r4[it, z] = m4[it, z]
        stage4[it] = [
            send(
                m4.at[it, (z + d) % 8], r4.at[it, z], s4_s.at[it, d], s4_r.at[it, d],
                place(((z + d) % 8) * 16 + e_me, x),
            )
            for d in FAR_8
        ]

    put_spectrum(0, spectrum)
    halo = send_halo(0)
    grams[0, 0] = dot_pairs(field, field)

    for it in range(KRYLOV):
        for q in range(4):
            for cl in range(2):
                h[q, 3 + cl, 4:12, :] = own[it, q, cl]
        for copy in halo[4:]:
            copy.wait_recv()
        for q in range(4):
            h[q, 0, 4:12, :] = left2[it, q]
            h[q, 7, 4:12, :] = right2[it, q]
            for cl in range(2):
                h[q, 1 + cl, 4:12, :] = left1[it, q, cl]
                h[q, 5 + cl, 4:12, :] = right1[it, q, cl]
                h[q, 3 + cl, 0:4, :] = north[it, q, cl]
                h[q, 3 + cl, 12:16, :] = south[it, q, cl]

        def first_guess(j, carry):
            guess_on(j, 0, 8)
            guess_on(j, 8, 8)
            return carry

        lax.fori_loop(0, 8, first_guess, 0, unroll=2)
        for copy in halo[:4]:
            copy.wait_recv()
        for cl in range(2):
            for q in range(4):
                h[q, 1 + cl, 2:4, :] = nw[it, q, cl]
                h[q, 1 + cl, 12:14, :] = sw[it, q, cl]
                h[q, 5 + cl, 2:4, :] = ne[it, q, cl]
                h[q, 5 + cl, 12:14, :] = se[it, q, cl]
            for j in (1 + cl, 5 + cl):
                for first in (2, 12):
                    guess_on(j, first, 2)
        sweep(wa, wb, 1, 7)
        sweep(wb, wa, 2, 6)
        guess, image = [], []
        for cl in range(2):
            j = 3 + cl
            w_row, g_row = [None] * 4, [None] * 4
            weights = weights_of(j, 4)
            for q in range(2):
                s_re, s_im, s_x = shifts[q]
                w_re, b_re = stencil(wa, q, j, 12, weights)
                w_im, b_im = stencil(wa, q + 2, j, 12, weights)
                w_row[q], w_row[q + 2] = w_re, w_im
                g_row[q] = b_re - (s_re * w_re + s_x * w_im)
                g_row[q + 2] = b_im - (s_im * w_im - s_x * w_re)
            mean = w_row[0] * small_ref[6:7, :]
            for q in range(1, 4):
                mean = mean + w_row[q] * small_ref[6 + q : 7 + q, :]
            corner = jnp.broadcast_to(jnp.sum(mean, axis=1, keepdims=True), (8, 128))
            g_row[0] = g_row[0] + corner
            g_row[1] = g_row[1] + corner
            g_row[2] = g_row[2] + jnp.where(lanes_below(1), corner, 0.0)
            guess.append(jnp.concatenate(w_row, axis=1))
            image.append(jnp.concatenate(g_row, axis=1))
        guess = jnp.concatenate(guess, axis=0)
        image = jnp.concatenate(image, axis=0)
        if it + 1 < KRYLOV:
            put_spectrum(it + 1, image)
            halo = send_halo(it + 1)
        both = jnp.dot(
            jnp.concatenate([guess, image], axis=0), inv[...], precision=HIGHEST, preferred_element_type=F32
        )
        directions.append(both[0:16])
        vectors.append(both[16:32])
        if it + 1 < KRYLOV:
            send_strip(it)
        for i in range(it + 2):
            grams[i, it + 1] = dot_pairs(vectors[i], vectors[it + 1])
        if it == 1:
            send_steps(0)

    order = [(i, j) for i in range(KRYLOV + 1) for j in range(i, KRYLOV + 1)]
    row_is = lax.broadcasted_iota(jnp.int32, (16, 128), 0)
    lane_is = lax.broadcasted_iota(jnp.int32, (16, 128), 1)
    high = jnp.zeros((16, 128), F32)
    low = jnp.zeros((16, 128), F32)
    for n, key in enumerate(order):
        a, b = grams[key]
        high = jnp.where(row_is == n, jnp.concatenate([a, a], axis=0), high)
        low = jnp.where(row_is == n, jnp.concatenate([b, b], axis=0), low)
    for shift in (64, 32, 16, 8, 4, 2, 1):
        high, t = two_sum(high, pltpu.roll(high, shift, 1))
        low = low + pltpu.roll(low, shift, 1) + t
    packed = jnp.where(lane_is == row_is, high, jnp.where(lane_is == row_is + 16, low, 0.0))
    mine = jnp.sum(packed, axis=0, keepdims=True)

    def add_start(mine, src, dst, s_sem, r_sem, devices, me):
        src[...] = mine
        dst[me] = mine
        return [send(src, dst.at[me], s_sem.at[d], r_sem.at[d], device) for d, device in devices]

    def add_end(copies, dst):
        for copy in copies:
            copy.wait_recv()
        level = [(dst[i], None) for i in range(len(copies) + 1)]
        while len(level) > 1:
            following = []
            for (a, ea), (b, eb) in zip(level[::2], level[1::2]):
                s, t = two_sum(a, b)
                for extra in (ea, eb):
                    t = t if extra is None else t + extra
                following.append((s, t))
            level = following
        s, t = level[0]
        lane = lax.broadcasted_iota(jnp.int32, (1, 128), 1)
        return s + jnp.where((lane >= 16) & (lane < 32), pltpu.roll(t, 16, 1), 0.0)

    others = [
        (d * 4 + c, place(((z + d) % 8) * 16 + e_me, (x + c) % 4)) for d, c in FAR_32
    ]
    adds = add_start(mine, ars1, ar1, a1_s, a1_r, others, z * 4 + x)
    send_strip(2)
    send_steps(1)
    mine = add_end(adds, ar1)
    adds = add_start(mine, ars0, ar0, a0_s, a0_r, [(d, place(z * 16 + (e_me + d) % 16, x)) for d in FAR_16], e_me)
    send_steps(2)
    mine = add_end(adds, ar0)
    mine = jnp.broadcast_to(mine, (8, 128))
    gram = [[None] * (KRYLOV + 1) for _ in range(KRYLOV + 1)]
    for n, (i, j) in enumerate(order):
        value = (
            jnp.broadcast_to(mine[:, n : n + 1], (8, 128)),
            jnp.broadcast_to(mine[:, 16 + n : 17 + n], (8, 128)),
        )
        gram[i][j] = value
        gram[j][i] = value
    on_directions, on_vectors = krylov_weights(gram)

    for it in range(KRYLOV):
        for copy in stage4[it]:
            copy.wait_recv()
    sums = [[], []]
    for zz in range(8):
        total = on_directions[0] * r4[0, zz, 0]
        for it in range(1, KRYLOV):
            total = total + on_directions[it] * r4[it, zz, 0]
        sums[0].append(total)
        total = on_vectors[0] * m1[zz]
        for it in range(KRYLOV):
            total = total + on_vectors[it + 1] * r4[it, zz, 1]
        sums[1].append(total)
    for f in range(2):
        for t in range(4):
            for hh in range(2):
                value = None
                for k in range(4):
                    piece = turn(sums[f][hh * 4 + k], k * 32 - t * 32)
                    value = piece if value is None else jnp.where(lane_block(k), piece, value)
                out_ref[f, t, :, hh * 128 : hh * 128 + 128] = value
    for copy in started:
        copy.wait_send()


def per_device(right_side, diffusion, velocity):
    forward, inverse, small = tables()
    vmem = pl.BlockSpec(memory_space=pltpu.VMEM)
    hbm = pl.BlockSpec(memory_space=pltpu.HBM)

    def buffer(*shape):
        return pltpu.VMEM(shape, F32)

    def sems(*shape):
        return pltpu.SemaphoreType.DMA(shape)

    both = pl.pallas_call(
        kernel,
        out_shape=jax.ShapeDtypeStruct((2, *right_side.shape), F32),
        in_specs=[hbm] * 6,
        out_specs=vmem,
        scratch_shapes=[
            buffer(4, 8, 256), buffer(8, 256), buffer(2, 8, 256), buffer(16, 128), buffer(L, L), buffer(L, L),
            buffer(8, 8, 128), buffer(8, 8, 128), buffer(128, 128), buffer(16, 4, 128), buffer(16, 4, 128),
            buffer(3, 8, 256), buffer(3, 2, 8, 256),
            buffer(5, 8, 16, 128), buffer(3, 2, 8, 16, 128),
            buffer(3, 4, 2, 8, 128), buffer(3, 2, 4, 2, 4, 128), buffer(3, 2, 4, 2, 2, 128),
            buffer(4, 8, 16, 128),
            buffer(3, 4, 2, 8, 128), buffer(3, 4, 2, 8, 128), buffer(3, 4, 8, 128), buffer(3, 4, 8, 128),
            buffer(3, 4, 2, 4, 128), buffer(3, 4, 2, 4, 128),
            buffer(3, 4, 2, 2, 128), buffer(3, 4, 2, 2, 128), buffer(3, 4, 2, 2, 128), buffer(3, 4, 2, 2, 128),
            buffer(4, 8, 32, 128), buffer(4, 8, 32, 128),
            buffer(16, 1, 128), buffer(32, 1, 128), buffer(1, 128), buffer(1, 128),
            buffer(3, 16, 8, 128), buffer(3, 16, 8, 128), buffer(128, 128),
            buffer(3, 8, 2, 8, 128), buffer(3, 8, 2, 8, 128),
            sems(6), sems(4), sems(4), sems(8), sems(8), sems(16), sems(16), sems(3, 10), sems(3, 10),
            sems(16), sems(16), sems(32), sems(32),
            sems(3, 16), sems(3, 16), sems(3, 8), sems(3, 8),
        ],
        compiler_params=pltpu.CompilerParams(
            collective_id=0, has_side_effects=True, vmem_limit_bytes=40_000_000
        ),
    )(*[pltpu.with_memory_space_constraint(v, pltpu.HBM) for v in (right_side, diffusion, velocity, jnp.asarray(small), jnp.asarray(forward), jnp.asarray(inverse))])
    return both[0], both[1]


def solution(mesh):
    return jax.shard_map(
        per_device,
        mesh=mesh,
        in_specs=(P("tm", "space", None), P("space", None), P(None, "space", None)),
        out_specs=(P("tm", "space", None), P("tm", "space", None)),
        check_vma=False,
    )
```

```python
import math

import jax
import jax.numpy as jnp
import numpy as np
from jax import lax
from jax.experimental import pallas as pl
from jax.experimental.pallas import tpu as pltpu
from jax.sharding import PartitionSpec as P

L = 512
KRYLOV = 3
ALPHA = 0.05
DAMPING = 0.8
EPSILON = 1e-06
LOG_DECAY = math.log(ALPHA) / L
DECAY = math.exp(LOG_DECAY)
MESH = pl.DeviceIdType.MESH
HIGHEST = lax.Precision.HIGHEST
FAR_8 = (4, 3, 5, 2, 6, 1, 7)
FAR_32 = tuple((d, c) for c in (2, 1, 3, 0) for d in FAR_8 + (0,) if (d, c) != (0, 0))
FAR_16 = (8, 7, 9, 6, 10, 5, 11, 4, 12, 3, 13, 2, 14, 1, 15)
F32 = jnp.float32


def tables():
    n = np.arange(L)
    k = np.arange(L // 2)
    angle = 2.0 * np.pi * ((n[:, None] * k[None, :]) % L) / L
    real = np.cos(angle)
    imag = -np.sin(angle)
    imag[:, 0] = np.where(n % 2 == 0, 1.0, -1.0)
    packed = np.concatenate([real, imag], axis=1)
    scale = np.full(L, 2.0 / L)
    scale[0] = scale[L // 2] = 1.0 / L
    decays = DECAY ** n
    forward = packed * decays[:, None]
    inverse = (packed * scale[None, :]).T / decays[None, :]
    shift_real = DECAY * np.cos(2.0 * np.pi * k / L)
    shift_imag = DECAY * np.sin(2.0 * np.pi * k / L)
    shift_other = shift_real.copy()
    shift_other[0] = -DECAY
    shift_imag[0] = 0.0
    corner = np.concatenate([shift_real * scale[: L // 2], shift_imag * scale[L // 2 :]])
    corner[L // 2] = -DECAY / L
    rows = np.concatenate([shift_real, shift_other, shift_imag, corner]).reshape(10, 128)
    small = np.zeros((16, 128))
    small[:10] = rows
    return forward.astype(np.float32), inverse.astype(np.float32), small.astype(np.float32)


def two_sum(a, b):
    s = a + b
    t = s - a
    return s, (a - (s - t)) + (b - t)


def split(a):
    c = 4097.0 * a
    high = c - (c - a)
    return high, a - high


def two_prod(a, b):
    p = a * b
    ah, al = split(a)
    bh, bl = split(b)
    return p, ((ah * bh - p) + ah * bl + al * bh) + al * bl


def pair_div(a, b):
    safe = jnp.where(b[0] > 0.0, b[0], 1.0)
    q = jnp.where(b[0] > 0.0, a[0] / safe, 0.0)
    p, e = two_prod(q, b[0])
    rest = ((a[0] - p) - e) + (a[1] - q * b[1])
    r = jnp.where(b[0] > 0.0, rest / safe, 0.0)
    s = q + r
    return s, r - (s - q)


def pair_less(a, m, b):
    p, e = two_prod(m[0], b[0])
    e = e + (m[0] * b[1] + m[1] * b[0])
    s, t = two_sum(a[0], -p)
    t = t + (a[1] - e)
    h = s + t
    return h, t - (h - s)


def krylov_weights(gram):
    n = KRYLOV + 1
    lower = [[None] * n for _ in range(n)]
    norm = [None] * n
    cross = [[None] * n for _ in range(n)]
    for k in range(n):
        for i in range(k, n):
            value = gram[k][i]
            for m in range(k):
                value = pair_less(value, lower[i][m], cross[k][m])
            cross[i][k] = value
        head = cross[k][k]
        keep = head[0] > 0.0
        head = (jnp.where(keep, head[0], 0.0), jnp.where(keep, head[1], 0.0))
        norm[k] = head[0]
        for i in range(k + 1, n):
            lower[i][k] = pair_div(cross[i][k], head)
    low = [[None if v is None else v[0] for v in row] for row in lower]
    zero = jnp.zeros_like(norm[0])
    images = []
    for k in range(KRYLOV):
        image = [low[k + 1][i] for i in range(k + 1)] + [zero + 1.0]
        for m in range(k):
            for i in range(m + 2):
                image[i] = image[i] - low[k][m] * images[m][i]
        images.append(image)
    beta = jnp.sqrt(norm[0] + EPSILON)
    basis = [[1.0 / beta]]
    hessen = [[zero] * KRYLOV for _ in range(n)]
    for j in range(KRYLOV):
        work = [zero] * (j + 2)
        for k in range(j + 1):
            for i in range(k + 2):
                work[i] = work[i] + basis[j][k] * images[k][i]
        for i in range(j + 1):
            total = zero
            for k in range(i + 1):
                total = total + basis[i][k] * norm[k] * work[k]
            hessen[i][j] = total
        for i in range(j + 1):
            for k in range(i + 1):
                work[k] = work[k] - hessen[i][j] * basis[i][k]
        total = zero
        for k in range(j + 2):
            total = total + work[k] * work[k] * norm[k]
        length = jnp.sqrt(total + EPSILON)
        hessen[j + 1][j] = length
        basis.append([v / length for v in work])
    ortho = []
    upper = [[None] * KRYLOV for _ in range(KRYLOV)]
    for column in range(KRYLOV):
        current = [hessen[i][column] for i in range(n)]
        for row in range(column):
            factor = sum(ortho[row][i] * current[i] for i in range(n))
            upper[row][column] = factor
            current = [current[i] - factor * ortho[row][i] for i in range(n)]
        length = jnp.sqrt(sum(v * v for v in current))
        upper[column][column] = length
        ortho.append([v / length for v in current])
    values = [None] * KRYLOV
    for row in reversed(range(KRYLOV)):
        accum = ortho[row][0] * beta
        for later in range(row + 1, KRYLOV):
            accum = accum - upper[row][later] * values[later]
        values[row] = accum / upper[row][row]
    target = []
    for i in range(n):
        accum = beta if i == 0 else zero
        for j in range(KRYLOV):
            accum = accum - hessen[i][j] * values[j]
        target.append(accum)

    def on_p(weights):
        on_u = [zero] * len(weights)
        for j, weight in enumerate(weights):
            for k in range(len(basis[j])):
                if k < len(weights):
                    on_u[k] = on_u[k] + weight * basis[j][k]
        for k in reversed(range(len(weights))):
            for i in range(k):
                on_u[i] = on_u[i] - low[k][i] * on_u[k]
        return on_u

    return on_p(values), on_p(target)


def lanes_below(count, shape=(8, 128)):
    return lax.broadcasted_iota(jnp.int32, shape, len(shape) - 1) < count


def lane_block(index):
    lane = lax.broadcasted_iota(jnp.int32, (8, 128), 1)
    return (lane >= 32 * index) & (lane < 32 * index + 32)


def turn(value, amount):
    amount = amount % 128
    return value if amount == 0 else pltpu.roll(value, amount, 1)


def kernel(
    b_hbm, diff_hbm, vel_hbm, small_hbm, fwd_hbm, inv_hbm,
    out_ref,
    b_ref, diff_ref, vel_ref, small_ref, fwd, inv,
    m1, r1, buf1, m2, r2, cd, cv, point, lead, own, edge4, edge2, h,
    left1, right1, left2, right2, north, south, nw, ne, sw, se, wa, wb,
    ar0, ar1, ars0, ars1, m3, r3, buf2, m4, r4,
    const_sem, coef_s, coef_r, s1_s, s1_r, s2_s, s2_r, ha_s, ha_r, a0_s, a0_r, a1_s, a1_r,
    s3_s, s3_r, s4_s, s4_r,
):
    tm = lax.axis_index("tm")
    x = lax.axis_index("space")
    z = tm // 16
    e_me = tm % 16
    y = e_me // 2
    core = e_me % 2
    odd = z % 2
    ys = y + odd * (7 - 2 * y)
    g = (z * 8 + ys) * 2 + core

    def at_strip(index):
        index = (index + 128) % 128
        strip = index // 2
        zz = strip // 8
        yy = strip % 8
        yy = yy + (zz % 2) * (7 - 2 * yy)
        return zz * 16 + yy * 2 + index % 2

    def place(t, s):
        return {"tm": t, "space": s}

    up = (x + 3) % 4
    down = (x + 1) % 4
    loads = [
        pltpu.make_async_copy(src, dst, const_sem.at[i])
        for i, (src, dst) in enumerate(
            (
                (b_hbm, b_ref), (diff_hbm, diff_ref), (vel_hbm, vel_ref),
                (small_hbm, small_ref), (fwd_hbm, fwd), (inv_hbm, inv),
            )
        )
    ]
    loads[0].start()
    barrier = pltpu.get_barrier_semaphore()
    greet = [place(((z + d) % 8) * 16 + e_me, x) for d in FAR_8]
    greet += [place(z * 16 + (e_me + d) % 16, x) for d in FAR_16]
    greet += [place(tm, up), place(tm, down)]
    for d in (-1, 1):
        for s in (up, down):
            greet.append(place(at_strip(g + d), s))
    for device in greet:
        pl.semaphore_signal(barrier, inc=1, device_id=device, device_id_type=MESH)
    for copy in loads[1:]:
        copy.start()
    loads[0].wait()

    for zz in range(8):
        value = None
        for t in range(4):
            piece = turn(b_ref[t, :, (zz // 4) * 128 : (zz // 4) * 128 + 128], t * 32 - (zz % 4) * 32)
            value = piece if value is None else jnp.where(lane_block(t), piece, value)
        m1[zz] = value
    r1[z] = m1[z]
    loads[1].wait()
    loads[2].wait()

    pl.semaphore_wait(barrier, len(greet))

    started = []

    def drain(keep):
        while len(started) > keep:
            started.pop(0).wait_send()

    def send(src, dst, s_sem, r_sem, device):
        copy = pltpu.make_async_remote_copy(
            src_ref=src, dst_ref=dst, send_sem=s_sem, recv_sem=r_sem, device_id=device, device_id_type=MESH
        )
        copy.start()
        started.append(copy)
        return copy

    stage1 = [
        send(m1.at[(z + d) % 8], r1.at[z], s1_s.at[d], s1_r.at[d], place(((z + d) % 8) * 16 + e_me, x))
        for d in FAR_8
    ]
    coefs = [
        send(diff_ref, cd.at[2], coef_s.at[0], coef_r.at[0], place(tm, up)),
        send(vel_ref, cv.at[2], coef_s.at[1], coef_r.at[1], place(tm, up)),
        send(diff_ref, cd.at[0], coef_s.at[2], coef_r.at[2], place(tm, down)),
        send(vel_ref, cv.at[0], coef_s.at[3], coef_r.at[3], place(tm, down)),
    ]
    h[...] = jnp.zeros_like(h)
    wa[...] = jnp.zeros_like(wa)
    wb[...] = jnp.zeros_like(wb)
    cd[1] = diff_ref[...]
    cv[1] = vel_ref[...]
    loads[3].wait()
    for copy in stage1:
        copy.wait_recv()
    half = lanes_below(64, (16, 128))
    turned = jnp.transpose(r1[...].reshape(64, 128))
    buf1[:, 0:64] = turned
    for t in range(4):
        even = buf1[pl.ds(t * 32, 16, stride=2), :]
        other = buf1[pl.ds(t * 32 + 1, 16, stride=2), :]
        m2[:, t, :] = jnp.where(half, even, pltpu.roll(other, 64, 1))

    def strip_of(e):
        yy = e // 2
        return (yy + odd * (7 - 2 * yy)) * 2 + e % 2

    r2[e_me] = m2[strip_of(e_me)]
    stage2 = []
    for d in FAR_16:
        to = (e_me + d) % 16
        stage2.append(
            send(m2.at[strip_of(to)], r2.at[e_me], s2_s.at[d], s2_r.at[d], place(z * 16 + to, x))
        )

    for copy in coefs:
        copy.wait_recv()
    parts = []
    for prev, mine, after in (
        (cd[0], cd[1], cd[2]),
        (cv[0, 0], cv[1, 0], cv[2, 0]),
        (cv[0, 1], cv[1, 1], cv[2, 1]),
    ):
        parts += [prev[4:8], mine, after[0:4]]
    stacked = jnp.concatenate(parts, axis=0)
    row_at = lax.broadcasted_iota(jnp.int32, (256, 128), 0)
    for j in range(8):
        pick = jnp.where(row_at == 2 * g - 3 + j, 1.0, 0.0).astype(F32)
        spread = jnp.dot(stacked, pick, precision=HIGHEST, preferred_element_type=F32)
        diff = spread[0:16]
        v_col = spread[16:32]
        v_row = spread[32:48]
        diag = 1.0 + 4.0 * diff
        point[0, j] = diag
        point[1, j] = -diff - v_row
        point[2, j] = -diff + v_row
        point[3, j] = -diff - v_col
        point[4, j] = -diff + v_col
        row = 8 * x - 4 + lax.broadcasted_iota(jnp.int32, (16, 128), 0)
        column = 2 * g - 3 + j
        inside = (row >= 0) & (row < 32) & (column >= 0) & (column < 256)
        for q in range(2):
            d_i = small_ref[4 + q : 5 + q, :]
            for which, base in ((0, 0), (1, 2)):
                d_r = diag - small_ref[base + q : base + q + 1, :]
                scale = jnp.where(inside, DAMPING / (d_r * d_r + d_i * d_i), 0.0)
                lead[which, q, j] = d_r * scale
                if which == 0:
                    lead[2, q, j] = d_i * scale

    for copy in stage2:
        copy.wait_recv()
    turned = jnp.transpose(r2[...].reshape(64, 128))
    low64 = lanes_below(64)
    tiles = []
    for cl in range(2):
        row = []
        for a in range(4):
            v0 = turned[cl * 64 + a * 16 : cl * 64 + a * 16 + 8, :]
            v1 = turned[cl * 64 + a * 16 + 8 : cl * 64 + a * 16 + 16, :]
            row.append(jnp.concatenate([v0, v1], axis=1))
        tiles.append(jnp.concatenate(row, axis=1))
    field = jnp.concatenate(tiles, axis=0)
    loads[4].wait()
    loads[5].wait()
    spectrum = jnp.dot(field, fwd[...], precision=HIGHEST, preferred_element_type=F32)
    vectors = [field]
    directions = []

    def dot_pairs(a, b):
        high = low = None
        for cl in range(2):
            for q in range(4):
                va = a[cl * 8 : cl * 8 + 8, q * 128 : q * 128 + 128]
                vb = b[cl * 8 : cl * 8 + 8, q * 128 : q * 128 + 128]
                p, e = two_prod(va, vb)
                if high is None:
                    high, low = p, e
                else:
                    high, t = two_sum(high, p)
                    low = low + (t + e)
        for shift in (4, 2, 1):
            high, t = two_sum(high, pltpu.roll(high, shift, 0))
            low = low + pltpu.roll(low, shift, 0) + t
        return high, low

    grams = {}

    def put_spectrum(it, value):
        for q in range(4):
            for cl in range(2):
                own[it, q, cl] = value[cl * 8 : cl * 8 + 8, q * 128 : q * 128 + 128]
                edge4[it, 0, q, cl] = value[cl * 8 : cl * 8 + 4, q * 128 : q * 128 + 128]
                edge4[it, 1, q, cl] = value[cl * 8 + 4 : cl * 8 + 8, q * 128 : q * 128 + 128]
                edge2[it, 0, q, cl] = value[cl * 8 : cl * 8 + 2, q * 128 : q * 128 + 128]
                edge2[it, 1, q, cl] = value[cl * 8 + 6 : cl * 8 + 8, q * 128 : q * 128 + 128]

    def send_halo(it):
        n1, n2, p1, p2 = (at_strip(g - 1), at_strip(g - 2), at_strip(g + 1), at_strip(g + 2))
        moves = (
            (edge2.at[it, 1], nw.at[it], place(p1, down)),
            (edge2.at[it, 1], ne.at[it], place(n1, down)),
            (edge2.at[it, 0], sw.at[it], place(p1, up)),
            (edge2.at[it, 0], se.at[it], place(n1, up)),
            (own.at[it], left1.at[it], place(p1, x)),
            (own.at[it], right1.at[it], place(n1, x)),
            (edge4.at[it, 1], north.at[it], place(tm, down)),
            (edge4.at[it, 0], south.at[it], place(tm, up)),
            (own.at[it, :, 1], left2.at[it], place(p2, x)),
            (own.at[it, :, 0], right2.at[it], place(n2, x)),
        )
        return [
            send(src, dst, ha_s.at[it, i], ha_r.at[it, i], device)
            for i, (src, dst, device) in enumerate(moves)
        ]

    shifts = [
        [jnp.broadcast_to(small_ref[2 * k + q : 2 * k + q + 1, :], (8, 128)) for k in range(3)] for q in range(2)
    ]

    def weights_of(j, at):
        return [point[k, j, pl.ds(at, 8), :] for k in range(5)]

    def stencil(w, q, j, start, weights):
        here = w[q, j, pl.ds(start, 8), :]
        return here, (
            weights[0] * here
            + weights[1] * w[q, j, pl.ds(start - 1, 8), :]
            + weights[2] * w[q, j, pl.ds(start + 1, 8), :]
            + weights[3] * w[q, j - 1, pl.ds(start, 8), :]
            + weights[4] * w[q, j + 1, pl.ds(start, 8), :]
        )

    def sweep(source, target, first, last):
        def body(j, carry):
            done = []
            for at in (0, 8):
                weights = weights_of(j, at)
                for q in range(2):
                    s_re, s_im, s_x = shifts[q]
                    w_re, b_re = stencil(source, q, j, 8 + at, weights)
                    w_im, b_im = stencil(source, q + 2, j, 8 + at, weights)
                    rows = pl.ds(at, 8)
                    left_re = h[q, j, rows, :] - (b_re - (s_re * w_re + s_x * w_im))
                    left_im = h[q + 2, j, rows, :] - (b_im - (s_im * w_im - s_x * w_re))
                    p_re, p_im, p_x = lead[0, q, j, rows, :], lead[1, q, j, rows, :], lead[2, q, j, rows, :]
                    done.append((q, at, w_re + (p_re * left_re + p_x * left_im)))
                    done.append((q + 2, at, w_im + (p_im * left_im - p_x * left_re)))
            for q, at, value in done:
                target[q, j, pl.ds(8 + at, 8), :] = value
            return carry

        lax.fori_loop(first, last, body, 0, unroll=2)

    def guess_on(j, first, rows):
        at = pl.ds(first, rows)
        done = []
        for q in range(2):
            re, im = h[q, j, at, :], h[q + 2, j, at, :]
            p_re, p_im, p_x = lead[0, q, j, at, :], lead[1, q, j, at, :], lead[2, q, j, at, :]
            done.append((q, p_re * re + p_x * im))
            done.append((q + 2, p_im * im - p_x * re))
        for q, value in done:
            wa[q, j, pl.ds(8 + first, rows), :] = value

    strip_me = strip_of(e_me)
    stage3, stage4 = {}, {}

    def pieces(value):
        return [[value[cl * 8 : cl * 8 + 8, q * 128 : q * 128 + 128] for q in range(4)] for cl in range(2)]

    def send_strip(it):
        p0, p1 = pieces(directions[it]), pieces(vectors[it + 1])
        rows = []
        for cl in range(2):
            for a in range(4):
                f0, f1 = p0[cl][a], p1[cl][a]
                rows.append(jnp.where(low64, f0, pltpu.roll(f1, 64, 1)))
                rows.append(jnp.where(low64, pltpu.roll(f0, 64, 1), f1))
        turned = jnp.transpose(jnp.concatenate(rows, axis=0))
        for src in range(16):
            for f in range(2):
                m3[it, src, f * 4 : f * 4 + 4, :] = turned[f * 64 + src * 4 : f * 64 + src * 4 + 4, :]
        r3[it, strip_me] = m3[it, e_me]
        stage3[it] = []
        for d in FAR_16:
            to = (e_me + d) % 16
            stage3[it].append(
                send(m3.at[it, to], r3.at[it, strip_me], s3_s.at[it, d], s3_r.at[it, d], place(z * 16 + to, x))
            )

    def send_steps(it):
        for copy in stage3[it]:
            copy.wait_recv()
        for t in range(4):
            f0 = r3[it, :, t, :]
            f1 = r3[it, :, 4 + t, :]
            buf2[pl.ds(t * 32, 16, stride=2), :] = jnp.where(half, f0, pltpu.roll(f1, 64, 1))
            buf2[pl.ds(t * 32 + 1, 16, stride=2), :] = jnp.where(half, pltpu.roll(f0, 64, 1), f1)
        turned = jnp.transpose(buf2[...])
        for zz in range(8):
            for f in range(2):
                m4[it, zz, f] = turned[f * 64 + zz * 8 : f * 64 + zz * 8 + 8, :]
        r4[it, z] = m4[it, z]
        stage4[it] = [
            send(
                m4.at[it, (z + d) % 8], r4.at[it, z], s4_s.at[it, d], s4_r.at[it, d],
                place(((z + d) % 8) * 16 + e_me, x),
            )
            for d in FAR_8
        ]

    put_spectrum(0, spectrum)
    halo = send_halo(0)
    grams[0, 0] = dot_pairs(field, field)

    for it in range(KRYLOV):
        for q in range(4):
            for cl in range(2):
                h[q, 3 + cl, 4:12, :] = own[it, q, cl]
        for copy in halo[4:]:
            copy.wait_recv()
        for q in range(4):
            h[q, 0, 4:12, :] = left2[it, q]
            h[q, 7, 4:12, :] = right2[it, q]
            for cl in range(2):
                h[q, 1 + cl, 4:12, :] = left1[it, q, cl]
                h[q, 5 + cl, 4:12, :] = right1[it, q, cl]
                h[q, 3 + cl, 0:4, :] = north[it, q, cl]
                h[q, 3 + cl, 12:16, :] = south[it, q, cl]

        def first_guess(j, carry):
            guess_on(j, 0, 8)
            guess_on(j, 8, 8)
            return carry

        lax.fori_loop(0, 8, first_guess, 0, unroll=2)
        for copy in halo[:4]:
            copy.wait_recv()
        for cl in range(2):
            for q in range(4):
                h[q, 1 + cl, 2:4, :] = nw[it, q, cl]
                h[q, 1 + cl, 12:14, :] = sw[it, q, cl]
                h[q, 5 + cl, 2:4, :] = ne[it, q, cl]
                h[q, 5 + cl, 12:14, :] = se[it, q, cl]
            for j in (1 + cl, 5 + cl):
                for first in (2, 12):
                    guess_on(j, first, 2)
        sweep(wa, wb, 1, 7)
        sweep(wb, wa, 2, 6)
        guess, image = [], []
        for cl in range(2):
            j = 3 + cl
            w_row, g_row = [None] * 4, [None] * 4
            weights = weights_of(j, 4)
            for q in range(2):
                s_re, s_im, s_x = shifts[q]
                w_re, b_re = stencil(wa, q, j, 12, weights)
                w_im, b_im = stencil(wa, q + 2, j, 12, weights)
                w_row[q], w_row[q + 2] = w_re, w_im
                g_row[q] = b_re - (s_re * w_re + s_x * w_im)
                g_row[q + 2] = b_im - (s_im * w_im - s_x * w_re)
            mean = w_row[0] * small_ref[6:7, :]
            for q in range(1, 4):
                mean = mean + w_row[q] * small_ref[6 + q : 7 + q, :]
            corner = jnp.broadcast_to(jnp.sum(mean, axis=1, keepdims=True), (8, 128))
            g_row[0] = g_row[0] + corner
            g_row[1] = g_row[1] + corner
            g_row[2] = g_row[2] + jnp.where(lanes_below(1), corner, 0.0)
            guess.append(jnp.concatenate(w_row, axis=1))
            image.append(jnp.concatenate(g_row, axis=1))
        guess = jnp.concatenate(guess, axis=0)
        image = jnp.concatenate(image, axis=0)
        if it + 1 < KRYLOV:
            put_spectrum(it + 1, image)
            halo = send_halo(it + 1)
        both = jnp.dot(
            jnp.concatenate([guess, image], axis=0), inv[...], precision=HIGHEST, preferred_element_type=F32
        )
        directions.append(both[0:16])
        vectors.append(both[16:32])
        if it + 1 < KRYLOV:
            send_strip(it)
        for i in range(it + 2):
            grams[i, it + 1] = dot_pairs(vectors[i], vectors[it + 1])
        if it == 1:
            send_steps(0)

    order = [(i, j) for i in range(KRYLOV + 1) for j in range(i, KRYLOV + 1)]
    row_is = lax.broadcasted_iota(jnp.int32, (16, 128), 0)
    lane_is = lax.broadcasted_iota(jnp.int32, (16, 128), 1)
    high = jnp.zeros((16, 128), F32)
    low = jnp.zeros((16, 128), F32)
    for n, key in enumerate(order):
        a, b = grams[key]
        high = jnp.where(row_is == n, jnp.concatenate([a, a], axis=0), high)
        low = jnp.where(row_is == n, jnp.concatenate([b, b], axis=0), low)
    for shift in (64, 32, 16, 8, 4, 2, 1):
        high, t = two_sum(high, pltpu.roll(high, shift, 1))
        low = low + pltpu.roll(low, shift, 1) + t
    packed = jnp.where(lane_is == row_is, high, jnp.where(lane_is == row_is + 16, low, 0.0))
    mine = jnp.sum(packed, axis=0, keepdims=True)

    def add_start(mine, src, dst, s_sem, r_sem, devices, me):
        src[...] = mine
        dst[me] = mine
        return [send(src, dst.at[me], s_sem.at[d], r_sem.at[d], device) for d, device in devices]

    def add_end(copies, dst):
        for copy in copies:
            copy.wait_recv()
        level = [(dst[i], None) for i in range(len(copies) + 1)]
        while len(level) > 1:
            following = []
            for (a, ea), (b, eb) in zip(level[::2], level[1::2]):
                s, t = two_sum(a, b)
                for extra in (ea, eb):
                    t = t if extra is None else t + extra
                following.append((s, t))
            level = following
        s, t = level[0]
        lane = lax.broadcasted_iota(jnp.int32, (1, 128), 1)
        return s + jnp.where((lane >= 16) & (lane < 32), pltpu.roll(t, 16, 1), 0.0)

    others = [
        (d * 4 + c, place(((z + d) % 8) * 16 + e_me, (x + c) % 4)) for d, c in FAR_32
    ]
    adds = add_start(mine, ars1, ar1, a1_s, a1_r, others, z * 4 + x)
    send_strip(2)
    send_steps(1)
    mine = add_end(adds, ar1)
    adds = add_start(mine, ars0, ar0, a0_s, a0_r, [(d, place(z * 16 + (e_me + d) % 16, x)) for d in FAR_16], e_me)
    send_steps(2)
    drain(len(FAR_16) + len(FAR_8))
    mine = add_end(adds, ar0)
    mine = jnp.broadcast_to(mine, (8, 128))
    gram = [[None] * (KRYLOV + 1) for _ in range(KRYLOV + 1)]
    for n, (i, j) in enumerate(order):
        value = (
            jnp.broadcast_to(mine[:, n : n + 1], (8, 128)),
            jnp.broadcast_to(mine[:, 16 + n : 17 + n], (8, 128)),
        )
        gram[i][j] = value
        gram[j][i] = value
    on_directions, on_vectors = krylov_weights(gram)

    for it in range(KRYLOV):
        for copy in stage4[it]:
            copy.wait_recv()
    sums = [[], []]
    for zz in range(8):
        total = on_directions[0] * r4[0, zz, 0]
        for it in range(1, KRYLOV):
            total = total + on_directions[it] * r4[it, zz, 0]
        sums[0].append(total)
        total = on_vectors[0] * m1[zz]
        for it in range(KRYLOV):
            total = total + on_vectors[it + 1] * r4[it, zz, 1]
        sums[1].append(total)
    for f in range(2):
        for t in range(4):
            for hh in range(2):
                value = None
                for k in range(4):
                    piece = turn(sums[f][hh * 4 + k], k * 32 - t * 32)
                    value = piece if value is None else jnp.where(lane_block(k), piece, value)
                out_ref[f, t, :, hh * 128 : hh * 128 + 128] = value
    drain(0)


def per_device(right_side, diffusion, velocity):
    forward, inverse, small = tables()
    vmem = pl.BlockSpec(memory_space=pltpu.VMEM)
    hbm = pl.BlockSpec(memory_space=pltpu.HBM)

    def buffer(*shape):
        return pltpu.VMEM(shape, F32)

    def sems(*shape):
        return pltpu.SemaphoreType.DMA(shape)

    both = pl.pallas_call(
        kernel,
        out_shape=jax.ShapeDtypeStruct((2, *right_side.shape), F32),
        in_specs=[hbm] * 6,
        out_specs=vmem,
        scratch_shapes=[
            buffer(4, 8, 256), buffer(8, 256), buffer(2, 8, 256), buffer(16, 128), buffer(L, L), buffer(L, L),
            buffer(8, 8, 128), buffer(8, 8, 128), buffer(128, 128), buffer(16, 4, 128), buffer(16, 4, 128),
            buffer(3, 8, 256), buffer(3, 2, 8, 256),
            buffer(5, 8, 16, 128), buffer(3, 2, 8, 16, 128),
            buffer(3, 4, 2, 8, 128), buffer(3, 2, 4, 2, 4, 128), buffer(3, 2, 4, 2, 2, 128),
            buffer(4, 8, 16, 128),
            buffer(3, 4, 2, 8, 128), buffer(3, 4, 2, 8, 128), buffer(3, 4, 8, 128), buffer(3, 4, 8, 128),
            buffer(3, 4, 2, 4, 128), buffer(3, 4, 2, 4, 128),
            buffer(3, 4, 2, 2, 128), buffer(3, 4, 2, 2, 128), buffer(3, 4, 2, 2, 128), buffer(3, 4, 2, 2, 128),
            buffer(4, 8, 32, 128), buffer(4, 8, 32, 128),
            buffer(16, 1, 128), buffer(32, 1, 128), buffer(1, 128), buffer(1, 128),
            buffer(3, 16, 8, 128), buffer(3, 16, 8, 128), buffer(128, 128),
            buffer(3, 8, 2, 8, 128), buffer(3, 8, 2, 8, 128),
            sems(6), sems(4), sems(4), sems(8), sems(8), sems(16), sems(16), sems(3, 10), sems(3, 10),
            sems(16), sems(16), sems(32), sems(32),
            sems(3, 16), sems(3, 16), sems(3, 8), sems(3, 8),
        ],
        compiler_params=pltpu.CompilerParams(
            collective_id=0, has_side_effects=True, vmem_limit_bytes=40_000_000
        ),
    )(*[pltpu.with_memory_space_constraint(v, pltpu.HBM) for v in (right_side, diffusion, velocity, jnp.asarray(small), jnp.asarray(forward), jnp.asarray(inverse))])
    return both[0], both[1]


def solution(mesh):
    return jax.shard_map(
        per_device,
        mesh=mesh,
        in_specs=(P("tm", "space", None), P("space", None), P(None, "space", None)),
        out_specs=(P("tm", "space", None), P("tm", "space", None)),
        check_vma=False,
    )
```
